256 devices in a mesh: gx: 8 (over y, z_lo), gy: 32 (over z_hi, x, core).
Axes of the slice: x: 4, y: 4, z: 8 (z_hi: 4, z_lo: 2; z = z_hi * 2 + z_lo), core: 2. Of those that a mesh axis runs over, the one named last changes fastest.
Arguments:
- state: float32 [5, 8, 2048, 3072], P(None, None, 'gy', 'gx'), may hold values from -6 to 6
- driving: float32 [5, 8, 2048, 3072], P(None, None, 'gy', 'gx'), may hold values from -6 to 6
- rate: float32 [5, 8], replicated, may hold values from 1 to 6
- sound_square: float32 [8, 2048, 3072], P(None, 'gy', 'gx'), may hold values from 0.3 to 1
Outputs:
- nudged: float32 [5, 8, 2048, 3072], P(None, None, 'gy', 'gx')
The draws below stay inside these ranges and needn't reach their ends.
All inputs are finite; a program needn't handle non-finite values.
Results may differ from the reference program's by a relative error of at most 0.000064.
Values sent between devices are 32-bit elements; how exact they have to be, the bound alone decides.
A program may use at most 128 MiB of HBM per device.

```python
import math
import jax
import jax.numpy as jnp
from jax import lax

NFIELD = 5
MODES = 64
SUBSTEPS = 3
LEVELS = 8
NX = 3072
NY = 2048


def block_scale(key, dims, cuts, low, high):
    def one(axis_at, shards_of):
        steps = jax.random.uniform(jax.random.fold_in(jax.random.fold_in(key, 6), axis_at), (shards_of,), jnp.float32, low / len(cuts), high / len(cuts))
        return jnp.repeat(jnp.exp(steps), dims[axis_at] // shards_of).reshape((-1,) + (1,) * (len(dims) - axis_at - 1))

    level = one(*cuts[0])
    for cut in cuts[1:]:
        level = level * one(*cut)
    return level


def centred(key, dims, scale, limit, cuts=(), held_as=jnp.bfloat16):
    gain = block_scale(key, dims, cuts, -0.22, 0.18) if cuts else 1.0
    array = jax.random.normal(key, dims, jnp.float32) * scale * gain
    return jnp.minimum(jnp.maximum(array, -limit), limit).astype(held_as)


def setup_inputs(seed: int = 0) -> dict:
    splits = jax.random.split(jax.random.key(seed), 5)
    return {
        "state": centred(splits[0], (NFIELD, LEVELS, NY, NX), 1.0, 6.0, ((2, 32), (3, 8)), jnp.float32),
        "driving": centred(splits[1], (NFIELD, LEVELS, NY, NX), 1.0, 6.0, ((2, 32), (3, 8)), jnp.float32),
        "rate": jnp.clip(jnp.exp(jax.random.uniform(splits[2], (NFIELD, LEVELS), jnp.float32, math.log(1.0), math.log(6.0))), 1.0, 6.0),
        "sound_square": jnp.clip(jnp.exp(math.log(1.0) - 1.2039728 * jax.random.uniform(splits[3], (LEVELS, NY, NX), jnp.float32) ** block_scale(splits[3], (LEVELS, NY, NX), ((1, 32), (2, 8)), -0.2, 0.2)), 0.3, 1.0),
    }


courant = 0.5


def tables(count, size):
    index = jnp.arange(size, dtype=jnp.int32)
    order = jnp.arange(count, dtype=jnp.int32)
    freq = jnp.where(order < count // 2, order, order - count // 2 + 1)
    wrapped = (freq[:, None] * (2 * index[None, :] + 1)) % (2 * size)
    phase = jnp.pi * wrapped.astype(jnp.float32) / size
    basis = jnp.where(order[:, None] < count // 2, jnp.cos(phase), jnp.sin(phase))
    scaling = jnp.where(order == 0, 1.0 / size, 2.0 / size).astype(jnp.float32)
    return basis, basis * scaling[:, None]


def vertical(field):
    padded = jnp.pad(field, ((1, 1), (0, 0), (0, 0)))
    return 0.5 * (padded[2:] - padded[:-2])


def horizontal(field):
    padded = jnp.pad(field, ((0, 0), (1, 1), (1, 1)))
    across = 0.5 * (padded[:, 1:-1, 2:] - padded[:, 1:-1, :-2])
    along = 0.5 * (padded[:, 2:, 1:-1] - padded[:, :-2, 1:-1])
    return across, along


def substep(fields, sound_square):
    wind_u, wind_v, wind_w, press, theta = fields
    press_x, press_y = horizontal(press)
    new_u = wind_u - courant * press_x
    new_v = wind_v - courant * press_y
    new_w = wind_w - courant * vertical(press) + courant * theta
    u_x, _ = horizontal(new_u)
    _, v_y = horizontal(new_v)
    diverge = u_x + v_y + vertical(new_w)
    new_p = press - courant * sound_square * diverge
    new_t = theta - courant * new_w
    return (new_u, new_v, new_w, new_p, new_t)


def reference(state, driving, rate, sound_square):
    high = lax.Precision.HIGHEST
    basis_x, weight_x = tables(MODES, NX)
    basis_y, weight_y = tables(MODES, NY)
    difference = state - driving
    partial_value = jnp.einsum('flyx,kx->flyk', difference, weight_x, precision=high)
    modes = jnp.einsum('flyk,jy->fljk', partial_value, weight_y, precision=high)
    scaled = rate[:, :, None, None] * modes
    rows_back = jnp.einsum('fljk,jy->flyk', scaled, basis_y, precision=high)
    tendency = jnp.einsum('flyk,kx->flyx', rows_back, basis_x, precision=high)
    fields = tuple(state[i] for i in range(NFIELD))
    for step in range(SUBSTEPS):
        fields = substep(fields, sound_square)
    advanced = jnp.stack(fields)
    return advanced - tendency
```

```python
import jax
import jax.numpy as jnp
from jax import lax
from jax.sharding import PartitionSpec as P

MODES = 64
SUBSTEPS = 3
GY = "gy"


courant = 0.5


def padded_2(cells, sides, width):
    for axis, dim in sides:
        count = lax.axis_size(axis)
        ends = count - 1
        head = lax.slice_in_dim(cells, 0, width, axis=dim)
        tail = lax.slice_in_dim(cells, cells.shape[dim] - width, cells.shape[dim], axis=dim)
        cells = jnp.concatenate(
            [
                lax.ppermute(tail, axis, [(i, (i + 1) % count) for i in range(ends)]),
                cells,
                lax.ppermute(head, axis, [((i + 1) % count, i) for i in range(ends)]),
            ],
            axis=dim,
        )
    return cells


def tables(count, size, offset, total):
    index = lax.iota(jnp.int32, size) + offset
    order = lax.iota(jnp.int32, count)
    freq = jnp.where(order < count // 2, order, order - count // 2 + 1)
    wrapped = freq[:, None] * (2 * index[None, :] + 1) % (2 * total)
    phase = jnp.pi * wrapped.astype(jnp.float32) / total
    basis = jnp.where(order[:, None] < count // 2, jnp.cos(phase), jnp.sin(phase))
    scaling = jnp.where(order == 0, 1.0 / total, 2.0 / total).astype(jnp.float32)
    return (basis, basis * scaling[:, None])


def vertical(field):
    padded = jnp.pad(field, ((1, 1), (0, 0), (0, 0)))
    return 0.5 * (padded[2:] - padded[:-2])


def inner(field):
    return field[..., 1:-1, 1:-1]


def window_step(fields, sound_square, inside):
    wind_u, wind_v, wind_w, press, theta = fields
    press_x = 0.5 * (press[:, 1:-1, 2:] - press[:, 1:-1, :-2])
    press_y = 0.5 * (press[:, 2:, 1:-1] - press[:, :-2, 1:-1])
    first = inner(inside)
    new_u = (inner(wind_u) - courant * press_x) * first
    new_v = (inner(wind_v) - courant * press_y) * first
    new_w = (inner(wind_w) - courant * vertical(inner(press)) + courant * inner(theta)) * first
    u_x = 0.5 * (new_u[:, 1:-1, 2:] - new_u[:, 1:-1, :-2])
    v_y = 0.5 * (new_v[:, 2:, 1:-1] - new_v[:, :-2, 1:-1])
    diverge = u_x + v_y + vertical(inner(new_w))
    second = inner(first)
    new_p = (inner(inner(press)) - courant * inner(inner(sound_square)) * diverge) * second
    new_t = (inner(inner(theta)) - courant * inner(new_w)) * second
    return (
        (inner(new_u) * second, inner(new_v) * second, inner(new_w) * second, new_p, new_t),
        inner(inner(sound_square)),
        second,
    )


def on_device(state, driving, rate, sound_square):
    high = lax.Precision.HIGHEST
    fields_count, levels, rows, cols = state.shape
    row_start = lax.axis_index(GY) * rows
    col_start = lax.axis_index("gx") * cols
    total_rows = rows * lax.axis_size(GY)
    total_cols = cols * lax.axis_size("gx")
    basis_x, weight_x = tables(MODES, cols, col_start, total_cols)
    basis_y, weight_y = tables(MODES, rows, row_start, total_rows)
    difference = state - driving
    partial_value = jnp.einsum("flyx,kx->flyk", difference, weight_x, precision=high)
    local = jnp.einsum("flyk,jy->fljk", partial_value, weight_y, precision=high)
    modes = lax.psum(local, ("gx", GY))
    scaled = rate[:, :, None, None] * modes
    rows_back = jnp.einsum("fljk,jy->flyk", scaled, basis_y, precision=high)
    tendency = jnp.einsum("flyk,kx->flyx", rows_back, basis_x, precision=high)
    margin = 2 * SUBSTEPS
    packed = jnp.concatenate([state, sound_square[None]], axis=0)
    widened = padded_2(packed, (("gx", 3), (GY, 2)), margin)
    row_ids = lax.iota(jnp.int32, rows + 2 * margin) + row_start - margin
    col_ids = lax.iota(jnp.int32, cols + 2 * margin) + col_start - margin
    row_ok = (row_ids >= 0) & (row_ids < total_rows)
    col_ok = (col_ids >= 0) & (col_ids < total_cols)
    inside = (row_ok[:, None] & col_ok[None, :]).astype(jnp.float32)
    fields = tuple((widened[i] for i in range(fields_count)))
    speeds = widened[fields_count]
    for step in range(SUBSTEPS):
        fields, speeds, inside = window_step(fields, speeds, inside)
    advanced = jnp.stack(fields)
    return advanced - tendency


def solution(mesh):
    return jax.shard_map(
        on_device,
        mesh=mesh,
        in_specs=(P(None, None, GY, "gx"), P(None, None, GY, "gx"), P(), P(None, GY, "gx")),
        out_specs=P(None, None, GY, "gx"),
        check_vma=False,
    )
```

```python
import jax
import jax.numpy as jnp
import numpy as np
from jax import lax
from jax.experimental import pallas as pl
from jax.experimental.pallas import tpu as pltpu
from jax.sharding import PartitionSpec as P

MODES = 64
SUBSTEPS = 3
NX = 3072
NY = 2048
NF, NL, ROWS, COLS = 5, 8, 64, 384
GX, GY = 8, 32
F32, BF16 = jnp.float32, jnp.bfloat16
MESH = pl.DeviceIdType.MESH
TOP, BOT = 16, 80
HALF, CHUNK = 640, 40
U, V, W, PR, TH, SS = range(6)


def basis(size):
    index = np.arange(size, dtype=np.int64)
    order = np.arange(MODES, dtype=np.int64)
    freq = np.where(order < MODES // 2, order, order - MODES // 2 + 1)
    wrapped = (freq[:, None] * (2 * index[None, :] + 1)) % (2 * size)
    phase = np.float32(np.pi) * wrapped.astype(np.float32) / np.float32(size)
    phase = phase.astype(np.float64)
    table = np.where(order[:, None] < MODES // 2, np.cos(phase), np.sin(phase))
    scaling = np.where(order == 0, 1.0 / size, 2.0 / size).astype(np.float32)
    table = table.astype(np.float32)
    return table, table * scaling[:, None]


def tables():
    basis_x, _ = basis(NX)
    basis_y, weight_y = basis(NY)
    tab_x = basis_x.reshape(MODES, GX, COLS).transpose(1, 0, 2)
    by_tile = basis_y.reshape(MODES, GY, ROWS).transpose(1, 2, 0)
    wy_tile = weight_y.reshape(MODES, GY, ROWS).transpose(1, 0, 2)
    return np.ascontiguousarray(tab_x), np.concatenate([wy_tile, by_tile], axis=2)


def lanes(shape):
    return lax.broadcasted_iota(jnp.int32, shape, len(shape) - 1)


def split(x):
    high = x.astype(BF16)
    return high, (x - high.astype(F32)).astype(BF16)


def y_table(pair):
    lane = lanes(pair.shape)
    high = pair.astype(BF16).astype(F32)
    first = jnp.where(lane < 64, high, pair - high)
    second = jnp.where(lane < 64, high, 0.0)
    return jnp.concatenate([first, second], axis=1).astype(BF16)


def dot(a, b):
    return jnp.dot(a, b, preferred_element_type=F32)


def mode_kernel(
    state, driving, sound, tab_x, tab_y,
    modes, adv, xt3, yt3,
    big, drv, tx, ty, wx, wy, mask, local, half, core_recv, xy_recv, red, z_recv,
    xs, xr, ys, yr, cs, cr,
    ld_sem, drv_sem, snd_sem, tab_sem, core_sem, xy_send, xy_got, z_send, z_got,
    ag_send, ag_got, fw_send, fw_got, xh_send, xh_got, yh_send, yh_got, ch_send, ch_got, out_sem,
):
    gx, gy = lax.axis_index("gx"), lax.axis_index("gy")
    py, zlo = gx // 2, gx % 2
    core, px, zhi = gy % 2, (gy // 2) % 4, gy // 8
    pz = zhi * 2 + zlo
    me = py * 4 + px

    def at(x, y, z, c):
        return {"gx": y * 2 + z % 2, "gy": ((z // 2) * 4 + x) * 2 + c}

    partner = at(px, py, pz, 1 - core)

    def plane(d):
        return (px + d % 4) % 4, (py + d // 4) % 4

    def plane_dev(d):
        x, y = plane(d)
        return at(x, y, pz, core)

    def column_dev(d):
        return at(px, py, (pz + d) % 8, core)

    left, right = {"gx": (gx + GX - 1) % GX, "gy": gy}, {"gx": (gx + 1) % GX, "gy": gy}
    above, below = {"gx": gx, "gy": (gy + GY - 1) % GY}, {"gx": gx, "gy": (gy + 1) % GY}
    sides = (left, right)
    rows_to = (above, below)

    far = sorted(range(1, 16), key=lambda d: -(min(d % 4, 4 - d % 4) + min(d // 4, 4 - d // 4)))
    deep = sorted(range(1, 8), key=lambda d: -min(d, 8 - d))

    barrier = pltpu.get_barrier_semaphore()
    peers = [partner] + [plane_dev(d) for d in far] + [column_dev(d) for d in deep]
    peers += [left, right, above, below]
    for peer in peers:
        pl.semaphore_signal(barrier, inc=1, device_id=peer, device_id_type=MESH)

    def remote(src, dst, send, recv, dev):
        return pltpu.make_async_remote_copy(
            src_ref=src, dst_ref=dst, send_sem=send, recv_sem=recv, device_id=dev, device_id_type=MESH
        )

    def load(f, t):
        return pltpu.make_async_copy(
            state.at[f, :, :, pl.ds(t * 128, 128)], big.at[f, :, t, pl.ds(TOP, ROWS), :], ld_sem.at[f, t]
        )

    def load_drv(f):
        return pltpu.make_async_copy(driving.at[f], drv.at[f], drv_sem.at[f])

    def load_sound(t):
        return pltpu.make_async_copy(
            sound.at[:, :, pl.ds(t * 128, 128)], big.at[SS, :, t, pl.ds(TOP, ROWS), :], snd_sem.at[t]
        )

    get_tx = pltpu.make_async_copy(tab_x.at[gx], tx, tab_sem.at[0])
    get_ty = pltpu.make_async_copy(tab_y.at[gy], ty, tab_sem.at[1])
    get_tx.start()
    get_ty.start()
    for f in range(NF):
        for t in range(3):
            load(f, t).start()
        load_drv(f).start()
    for t in range(3):
        load_sound(t).start()

    get_tx.wait()
    get_ty.wait()
    b_x = tx[...]
    k_row = lax.broadcasted_iota(jnp.int32, b_x.shape, 0)
    w_x = b_x * jnp.where(k_row == 0, np.float32(1.0 / NX), np.float32(2.0 / NX))
    w_hi, w_lo = split(w_x)
    wx[...] = jnp.concatenate([w_hi, w_hi, w_lo, w_lo], axis=0)
    b_hi, b_lo = split(b_x)
    xt3[...] = jnp.concatenate([b_hi, b_hi, b_hi, b_hi, b_lo, b_lo], axis=0)
    pair = ty[...]
    lane2 = lanes(pair.shape)
    turned = pltpu.roll(pair, 64, 1)
    wy[...] = y_table(jnp.where(lane2 < 64, pair, turned))
    yt3[...] = y_table(jnp.where(lane2 < 64, turned, pair))

    row = lax.broadcasted_iota(jnp.int32, (96, 128), 0)
    lane = lanes((96, 128))
    row_ok = ((row >= TOP) | (gy > 0)) & ((row < BOT) | (gy < GY - 1))
    col_ok = jnp.where(lane < 64, jnp.where(gx < GX - 1, 1.0, 0.0), jnp.where(gx > 0, 1.0, 0.0))
    row_ok = jnp.where(row_ok, 1.0, 0.0)
    for t in range(3):
        mask[t] = row_ok
    mask[3] = row_ok * col_ok

    def project(f, _):
        for t in range(3):
            load(f, t).wait()
        load_drv(f).wait()
        diff = jnp.concatenate(
            [
                big[f, :, t, TOP:BOT, :].reshape(512, 128)
                - drv[f, :, :, t * 128 : (t + 1) * 128].reshape(512, 128)
                for t in range(3)
            ],
            axis=1,
        )
        high, low = split(diff)
        nt = (((1,), (1,)), ((), ()))
        a = lax.dot_general(high, wx[...], nt, preferred_element_type=F32)
        b = lax.dot_general(low, wx[0:128], nt, preferred_element_type=F32)
        part = a[:, :128] + (a[:, 128:] + b)
        side = lanes((64, 128))
        pairs = [
            jnp.where(side < 64, part[128 * q : 128 * q + 64], part[128 * q + 64 : 128 * q + 128])
            for q in range(4)
        ]
        high, low = split(jnp.concatenate(pairs, axis=1))
        rhs = jnp.concatenate([high, high, low, low], axis=0)
        out = dot(wy[...], rhs)
        for q in range(4):
            local[pl.ds(pl.multiple_of((f * 4 + q) * 64, 64), 64), :] = out[:, 128 * q : 128 * q + 128]
        return 0

    lax.fori_loop(0, NF, project, 0)
    pl.semaphore_wait(barrier, len(peers))

    give = remote(
        local.at[pl.ds(pl.multiple_of((1 - core) * HALF, 8), HALF), :], core_recv, core_sem.at[0], core_sem.at[1], partner
    )
    give.start()

    for t in range(3):
        load_sound(t).wait()
    slot = lanes((32, 128)) // 8

    def pack_x(f, _):
        for side, tile in ((0, 0), (1, 2)):
            acc = None
            for i in range(16):
                cells = big[f, i // 2, tile, TOP + 32 * (i % 2) : TOP + 32 * (i % 2) + 32, :]
                shift = (8 * (i + side)) % 128
                cells = pltpu.roll(cells, shift, 1) if shift else cells
                acc = cells if acc is None else jnp.where(slot == i, cells, acc)
            xs[side, f] = acc
        return 0

    lax.fori_loop(0, 6, pack_x, 0)
    x_copies = [remote(xs.at[s], xr.at[s], xh_send.at[s], xh_got.at[s], sides[s]) for s in range(2)]
    for copy in x_copies:
        copy.start()

    give.wait()
    half[...] = local[pl.ds(pl.multiple_of(core * HALF, 8), HALF), :] + core_recv[...]

    def scatter(d):
        x, y = plane(d)
        return remote(
            half.at[pl.ds(pl.multiple_of((y * 4 + x) * CHUNK, 8), CHUNK), :],
            xy_recv.at[d], xy_send.at[d], xy_got.at[d], plane_dev(d),
        )

    for d in far:
        scatter(d).start()

    low_rows = lax.broadcasted_iota(jnp.int32, (3, 8, 128), 1) < 4

    def pack_y(l, _):
        for s, r in ((0, TOP), (1, BOT - 8)):
            def strip(f):
                return big[f, l, 0:3, r : r + 8, :]

            def joined(a, b):
                if s == 0:
                    return jnp.where(low_rows, strip(a), pltpu.roll(strip(b), 4, 1))
                return jnp.where(low_rows, pltpu.roll(strip(a), 4, 1), strip(b))

            ys[s, l, 0] = strip(PR)
            ys[s, l, 1] = strip(V)
            ys[s, l, 2] = joined(U, W)
            ys[s, l, 3] = joined(TH, SS)
        return 0

    lax.fori_loop(0, NL, pack_y, 0)
    y_copies = [remote(ys.at[s], yr.at[s], yh_send.at[s], yh_got.at[s], rows_to[s]) for s in range(2)]
    for copy in y_copies:
        copy.start()

    for copy in x_copies:
        copy.wait()
    near = lanes((32, 128)) < 64

    def unpack_x(f, _):
        for i in range(16):
            shift_a, shift_b = (128 - 8 * i) % 128, (128 - 8 * (i + 1)) % 128
            a, b = xr[0, f], xr[1, f]
            a = pltpu.roll(a, shift_a, 1) if shift_a else a
            b = pltpu.roll(b, shift_b, 1) if shift_b else b
            r = TOP + 32 * (i % 2)
            big[f, i // 2, 3, r : r + 32, :] = jnp.where(near, a, b)
        return 0

    lax.fori_loop(0, 6, unpack_x, 0)

    slot8 = lanes((8, 128)) // 16

    def pack_c(f, _):
        for s, r in ((0, TOP), (1, BOT - 8)):
            acc = None
            for l in range(NL):
                shift = (8 + 16 * l) % 128
                cells = pltpu.roll(big[f, l, 3, r : r + 8, :], shift, 1)
                acc = cells if acc is None else jnp.where(slot8 == l, cells, acc)
            cs[s, f] = acc
        return 0

    lax.fori_loop(0, 6, pack_c, 0)
    c_copies = [remote(cs.at[s], cr.at[s], ch_send.at[s], ch_got.at[s], rows_to[s]) for s in range(2)]
    for copy in c_copies:
        copy.start()

    for d in far:
        scatter(d).wait_recv()
    total = half[pl.ds(pl.multiple_of(me * CHUNK, 8), CHUNK), :]
    for d in range(1, 16):
        total = total + xy_recv[d]
    red[...] = total

    def across(d):
        return remote(red, z_recv.at[d], z_send.at[d], z_got.at[d], column_dev(d))

    for d in deep:
        across(d).start()
    for d in deep:
        across(d).wait_recv()
    total = red[...]
    for d in range(1, 8):
        total = total + z_recv[d]

    def chunk_of(q):
        return modes.at[pl.ds(pl.multiple_of(core * HALF + q * CHUNK, 8), CHUNK), :]

    modes[pl.ds(pl.multiple_of(core * HALF + me * CHUNK, 8), CHUNK), :] = total

    def gather(d):
        return remote(chunk_of(me), chunk_of(me), ag_send.at[d], ag_got.at[d], plane_dev(d))

    def forward(d):
        x, y = (px + 4 - d % 4) % 4, (py + 4 - d // 4) % 4
        ref = chunk_of(y * 4 + x)
        return remote(ref, ref, fw_send.at[d], fw_got.at[d], partner)

    for d in far:
        gather(d).start()
    forward(0).start()

    for copy in y_copies:
        copy.wait()
    for copy in c_copies:
        copy.wait()

    def unpack_y(l, _):
        for s, r in ((0, BOT), (1, TOP - 8)):
            def put(f, cells):
                big[f, l, 0:3, r : r + 8, :] = cells

            def other(cells):
                return pltpu.roll(cells, 4, 1)

            put(PR, yr[s, l, 0] * mask[0:3, r : r + 8, :])
            put(V, yr[s, l, 1])
            one, two = yr[s, l, 2], yr[s, l, 3]
            if s == 0:
                put(U, one)
                put(W, other(one))
                put(TH, two)
                put(SS, other(two))
            else:
                put(U, other(one))
                put(W, one)
                put(TH, other(two))
                put(SS, two)
        return 0

    lax.fori_loop(0, NL, unpack_y, 0)

    def unpack_c(f, _):
        for s, r in ((0, BOT), (1, TOP - 8)):
            for l in range(NL):
                big[f, l, 3, r : r + 8, :] = pltpu.roll(cr[s, f], (128 - 8 - 16 * l) % 128, 1)
        return 0

    lax.fori_loop(0, 6, unpack_c, 0)

    def mask_p(l, _):
        big[PR, l, 3, 8:88, :] = big[PR, l, 3, 8:88, :] * mask[3, 8:88, :]
        return 0

    lax.fori_loop(0, NL, mask_p, 0)

    lane4 = lanes((4, 16, 128))
    at_end, at_start = lane4 == 127, lane4 == 0

    def across_x(c):
        fwd, back = pltpu.roll(c, 127, 2), pltpu.roll(c, 1, 2)
        fwd = jnp.where(at_end, jnp.concatenate([fwd[1:], fwd[:1]], axis=0), fwd)
        back = jnp.where(at_start, jnp.concatenate([back[3:], back[:3]], axis=0), back)
        return fwd - back

    def get(f, l, r):
        return big[f, l, :, r : r + 16, :]

    def vertical(f, l, r):
        up = get(f, jnp.minimum(l + 1, NL - 1), r) * jnp.where(l < NL - 1, 1.0, 0.0)
        down = get(f, jnp.maximum(l - 1, 0), r) * jnp.where(l > 0, 1.0, 0.0)
        return up - down

    def winds(l, _):
        for r in range(8, 88, 16):
            ok = mask[:, r : r + 16, :]
            big[U, l, :, r : r + 16, :] = (get(U, l, r) - 0.25 * across_x(get(PR, l, r))) * ok
            along = get(PR, l, r + 1) - get(PR, l, r - 1)
            big[V, l, :, r : r + 16, :] = (get(V, l, r) - 0.25 * along) * ok
            big[W, l, :, r : r + 16, :] = get(W, l, r) - 0.25 * vertical(PR, l, r) + 0.5 * get(TH, l, r)
        return 0

    def pressure(rows):
        def body(l, _):
            for r in rows:
                along = get(V, l, r + 1) - get(V, l, r - 1)
                diverge = across_x(get(U, l, r)) + along + vertical(W, l, r)
                new_p = (get(PR, l, r) - 0.25 * get(SS, l, r) * diverge) * mask[:, r : r + 16, :]
                big[PR, l, :, r : r + 16, :] = new_p
                big[TH, l, :, r : r + 16, :] = get(TH, l, r) - 0.5 * get(W, l, r)
            return 0

        return body

    def put_out(first, count, t, k):
        return pltpu.make_async_copy(
            big.at[pl.ds(first, count), :, t, pl.ds(TOP, ROWS), :],
            adv.at[pl.ds(first, count), :, :, pl.ds(t * 128, 128)],
            out_sem.at[k, t],
        )

    for step in range(SUBSTEPS):
        last = step == SUBSTEPS - 1
        lax.fori_loop(0, NL, winds, 0)
        if last:
            for t in range(3):
                put_out(0, 3, t, 0).start()
            for d in far:
                gather(d).wait_recv()
                forward(d).start()
        lax.fori_loop(0, NL, pressure(range(TOP, BOT, 16) if last else range(8, 88, 16)), 0)
    for t in range(3):
        put_out(3, 2, t, 1).start()

    for d in range(16):
        forward(d).wait()
    for d in far:
        scatter(d).wait_send()
        gather(d).wait_send()
    for d in deep:
        across(d).wait_send()
    for t in range(3):
        put_out(0, 3, t, 0).wait()
        put_out(3, 2, t, 1).wait()


def sum_modes(state, driving, sound, tab_x, tab_y):
    vmem = pl.BlockSpec(memory_space=pltpu.VMEM)
    hbm = pl.BlockSpec(memory_space=pl.ANY)
    dma = pltpu.SemaphoreType.DMA
    return pl.pallas_call(
        mode_kernel,
        out_shape=(
            jax.ShapeDtypeStruct((2 * HALF, 128), F32),
            jax.ShapeDtypeStruct((NF, NL, ROWS, COLS), F32),
            jax.ShapeDtypeStruct((384, COLS), BF16),
            jax.ShapeDtypeStruct((64, 256), BF16),
        ),
        in_specs=[hbm] * 5,
        out_specs=(vmem, hbm, vmem, vmem),
        scratch_shapes=[
            pltpu.VMEM((6, NL, 4, 96, 128), F32),
            pltpu.VMEM((NF, NL, ROWS, COLS), F32),
            pltpu.VMEM((MODES, COLS), F32),
            pltpu.VMEM((64, 128), F32),
            pltpu.VMEM((256, COLS), BF16),
            pltpu.VMEM((64, 256), BF16),
            pltpu.VMEM((4, 96, 128), F32),
            pltpu.VMEM((2 * HALF, 128), F32),
            pltpu.VMEM((HALF, 128), F32),
            pltpu.VMEM((HALF, 128), F32),
            pltpu.VMEM((16, CHUNK, 128), F32),
            pltpu.VMEM((CHUNK, 128), F32),
            pltpu.VMEM((8, CHUNK, 128), F32),
            pltpu.VMEM((2, 6, 32, 128), F32),
            pltpu.VMEM((2, 6, 32, 128), F32),
            pltpu.VMEM((2, NL, 4, 3, 8, 128), F32),
            pltpu.VMEM((2, NL, 4, 3, 8, 128), F32),
            pltpu.VMEM((2, 6, 8, 128), F32),
            pltpu.VMEM((2, 6, 8, 128), F32),
            dma((NF, 3)), dma((NF,)), dma((3,)), dma((2,)), dma((2,)),
            dma((16,)), dma((16,)), dma((8,)), dma((8,)),
            dma((16,)), dma((16,)), dma((16,)), dma((16,)),
            dma((2,)), dma((2,)), dma((2,)), dma((2,)), dma((2,)), dma((2,)), dma((2, 3)),
        ],
        compiler_params=pltpu.CompilerParams(
            collective_id=0, has_side_effects=True, vmem_limit_bytes=48 * 1024 * 1024
        ),
        name="sum_modes",
    )(state, driving, sound, tab_x, tab_y)


def back_kernel(rate, modes, xt3, yt3, adv, out):
    f = pl.program_id(0)
    side = lanes((64, 128)) < 64
    scaled = [modes[q] * jnp.where(side, rate[f, 2 * q], rate[f, 2 * q + 1]) for q in range(4)]
    high, low = split(jnp.concatenate(scaled, axis=1))
    back = dot(yt3[...], jnp.concatenate([high, high, low, low], axis=0))
    rows = []
    for q in range(4):
        both = back[:, 128 * q : 128 * q + 128]
        rows += [jnp.where(side, both, 0.0), jnp.where(side, 0.0, both)]
    high, low = split(jnp.concatenate(rows, axis=0))
    tendency = dot(jnp.concatenate([high, low, high], axis=1), xt3[...])
    out[0] = adv[0] - tendency.reshape(NL, ROWS, COLS)


def nudge(rate, modes, xt3, yt3, adv):
    block = pl.BlockSpec((1, NL, ROWS, COLS), lambda f: (f, 0, 0, 0))
    vmem = pl.BlockSpec(memory_space=pltpu.VMEM)
    return pl.pallas_call(
        back_kernel,
        grid=(NF,),
        out_shape=jax.ShapeDtypeStruct((NF, NL, ROWS, COLS), F32),
        in_specs=[
            pl.BlockSpec(memory_space=pltpu.SMEM),
            pl.BlockSpec((4, 64, 128), lambda f: (f, 0, 0)),
            vmem,
            vmem,
            block,
        ],
        out_specs=block,
        compiler_params=pltpu.CompilerParams(
            dimension_semantics=("arbitrary",), vmem_limit_bytes=24 * 1024 * 1024
        ),
        name="nudge",
    )(rate, modes, xt3, yt3, adv)


def solution(mesh):
    tab_x, tab_y = tables()

    def on_device(state, driving, rate, sound_square):
        modes, adv, xt3, yt3 = sum_modes(state, driving, sound_square, jnp.asarray(tab_x), jnp.asarray(tab_y))
        return nudge(rate, modes.reshape(20, 64, 128), xt3, yt3, adv)

    return jax.shard_map(
        on_device,
        mesh=mesh,
        in_specs=(P(None, None, "gy", "gx"), P(None, None, "gy", "gx"), P(), P(None, "gy", "gx")),
        out_specs=P(None, None, "gy", "gx"),
        check_vma=False,
    )
```

```python
import jax
import jax.numpy as jnp
import numpy as np
from jax import lax
from jax.experimental import pallas as pl
from jax.experimental.pallas import tpu as pltpu
from jax.sharding import PartitionSpec as P

MODES = 64
SUBSTEPS = 3
NX = 3072
NY = 2048
NF, NL, ROWS, COLS = 5, 8, 64, 384
GX, GY = 8, 32
F32, BF16 = jnp.float32, jnp.bfloat16
MESH = pl.DeviceIdType.MESH
TOP, BOT = 16, 80
HALF, CHUNK = 640, 40
U, V, W, PR, TH, SS = range(6)


def basis(size):
    index = np.arange(size, dtype=np.int64)
    order = np.arange(MODES, dtype=np.int64)
    freq = np.where(order < MODES // 2, order, order - MODES // 2 + 1)
    wrapped = (freq[:, None] * (2 * index[None, :] + 1)) % (2 * size)
    phase = np.float32(np.pi) * wrapped.astype(np.float32) / np.float32(size)
    phase = phase.astype(np.float64)
    table = np.where(order[:, None] < MODES // 2, np.cos(phase), np.sin(phase))
    scaling = np.where(order == 0, 1.0 / size, 2.0 / size).astype(np.float32)
    table = table.astype(np.float32)
    return table, table * scaling[:, None]


def tables():
    basis_x, _ = basis(NX)
    basis_y, weight_y = basis(NY)
    tab_x = basis_x.reshape(MODES, GX, COLS).transpose(1, 0, 2)
    by_tile = basis_y.reshape(MODES, GY, ROWS).transpose(1, 2, 0)
    wy_tile = weight_y.reshape(MODES, GY, ROWS).transpose(1, 0, 2)
    return np.ascontiguousarray(tab_x), np.concatenate([wy_tile, by_tile], axis=2)


def lanes(shape):
    return lax.broadcasted_iota(jnp.int32, shape, len(shape) - 1)


def split(x):
    high = x.astype(BF16)
    return high, (x - high.astype(F32)).astype(BF16)


def y_table(pair):
    lane = lanes(pair.shape)
    high = pair.astype(BF16).astype(F32)
    first = jnp.where(lane < 64, high, pair - high)
    second = jnp.where(lane < 64, high, 0.0)
    return jnp.concatenate([first, second], axis=1).astype(BF16)


def dot(a, b):
    return jnp.dot(a, b, preferred_element_type=F32)


def mode_kernel(
    state, driving, sound, tab_x, tab_y,
    modes, adv, xt3, yt3,
    big, drv, tx, ty, wx, wy, mask, local, half, core_recv, xy_recv, red, z_recv,
    xs, xr, ys, yr, cs, cr,
    ld_sem, drv_sem, snd_sem, tab_sem, core_sem, xy_send, xy_got, z_send, z_got,
    ag_send, ag_got, fw_send, fw_got, xh_send, xh_got, yh_send, yh_got, ch_send, ch_got,
):
    gx, gy = lax.axis_index("gx"), lax.axis_index("gy")
    py, zlo = gx // 2, gx % 2
    core, px, zhi = gy % 2, (gy // 2) % 4, gy // 8
    pz = zhi * 2 + zlo
    me = py * 4 + px

    def at(x, y, z, c):
        return {"gx": y * 2 + z % 2, "gy": ((z // 2) * 4 + x) * 2 + c}

    partner = at(px, py, pz, 1 - core)

    def plane(d):
        return (px + d % 4) % 4, (py + d // 4) % 4

    def plane_dev(d):
        x, y = plane(d)
        return at(x, y, pz, core)

    def column_dev(d):
        return at(px, py, (pz + d) % 8, core)

    left, right = {"gx": (gx + GX - 1) % GX, "gy": gy}, {"gx": (gx + 1) % GX, "gy": gy}
    above, below = {"gx": gx, "gy": (gy + GY - 1) % GY}, {"gx": gx, "gy": (gy + 1) % GY}
    sides = (left, right)
    rows_to = (above, below)

    far = sorted(range(1, 16), key=lambda d: -(min(d % 4, 4 - d % 4) + min(d // 4, 4 - d // 4)))
    deep = sorted(range(1, 8), key=lambda d: -min(d, 8 - d))

    barrier = pltpu.get_barrier_semaphore()
    peers = [partner] + [plane_dev(d) for d in far] + [column_dev(d) for d in deep]
    peers += [left, right, above, below]
    for peer in peers:
        pl.semaphore_signal(barrier, inc=1, device_id=peer, device_id_type=MESH)

    def remote(src, dst, send, recv, dev):
        return pltpu.make_async_remote_copy(
            src_ref=src, dst_ref=dst, send_sem=send, recv_sem=recv, device_id=dev, device_id_type=MESH
        )

    def load(f, t):
        return pltpu.make_async_copy(
            state.at[f, :, :, pl.ds(t * 128, 128)], big.at[f, :, t, pl.ds(TOP, ROWS), :], ld_sem.at[f, t]
        )

    def load_drv(f):
        return pltpu.make_async_copy(driving.at[f], drv.at[f], drv_sem.at[f])

    def load_sound(t):
        return pltpu.make_async_copy(
            sound.at[:, :, pl.ds(t * 128, 128)], big.at[SS, :, t, pl.ds(TOP, ROWS), :], snd_sem.at[t]
        )

    get_tx = pltpu.make_async_copy(tab_x.at[gx], tx, tab_sem.at[0])
    get_ty = pltpu.make_async_copy(tab_y.at[gy], ty, tab_sem.at[1])
    get_tx.start()
    get_ty.start()
    def nth(i):
        return jnp.where(core == 0, NF - 1 - i, i)

    for i in range(NF):
        for t in range(3):
            load(nth(i), t).start()
        load_drv(nth(i)).start()
    for t in range(3):
        load_sound(t).start()

    get_tx.wait()
    get_ty.wait()
    b_x = tx[...]
    k_row = lax.broadcasted_iota(jnp.int32, b_x.shape, 0)
    w_x = b_x * jnp.where(k_row == 0, np.float32(1.0 / NX), np.float32(2.0 / NX))
    w_hi, w_lo = split(w_x)
    wx[...] = jnp.concatenate([w_hi, w_hi, w_lo, w_lo], axis=0)
    b_hi, b_lo = split(b_x)
    xt3[...] = jnp.concatenate([b_hi, b_hi, b_hi, b_hi, b_lo, b_lo], axis=0)
    pair = ty[...]
    lane2 = lanes(pair.shape)
    turned = pltpu.roll(pair, 64, 1)
    wy[...] = y_table(jnp.where(lane2 < 64, pair, turned))
    yt3[...] = y_table(jnp.where(lane2 < 64, turned, pair))

    row = lax.broadcasted_iota(jnp.int32, (96, 128), 0)
    lane = lanes((96, 128))
    row_ok = ((row >= TOP) | (gy > 0)) & ((row < BOT) | (gy < GY - 1))
    col_ok = jnp.where(lane < 64, jnp.where(gx < GX - 1, 1.0, 0.0), jnp.where(gx > 0, 1.0, 0.0))
    row_ok = jnp.where(row_ok, 1.0, 0.0)
    for t in range(3):
        mask[t] = row_ok
    mask[3] = row_ok * col_ok

    def project(i, _):
        f = nth(i)
        for t in range(3):
            load(f, t).wait()
        load_drv(f).wait()
        diff = jnp.concatenate(
            [
                big[f, :, t, TOP:BOT, :].reshape(512, 128)
                - drv[f, :, :, t * 128 : (t + 1) * 128].reshape(512, 128)
                for t in range(3)
            ],
            axis=1,
        )
        high, low = split(diff)
        nt = (((1,), (1,)), ((), ()))
        a = lax.dot_general(high, wx[...], nt, preferred_element_type=F32)
        b = lax.dot_general(low, wx[0:128], nt, preferred_element_type=F32)
        part = a[:, :128] + (a[:, 128:] + b)
        side = lanes((64, 128))
        pairs = [
            jnp.where(side < 64, part[128 * q : 128 * q + 64], part[128 * q + 64 : 128 * q + 128])
            for q in range(4)
        ]
        high, low = split(jnp.concatenate(pairs, axis=1))
        rhs = jnp.concatenate([high, high, low, low], axis=0)
        out = dot(wy[...], rhs)
        for q in range(4):
            local[pl.ds(pl.multiple_of((f * 4 + q) * 64, 64), 64), :] = out[:, 128 * q : 128 * q + 128]
        return 0

    lax.fori_loop(0, 3, project, 0)
    pl.semaphore_wait(barrier, len(peers))

    give = remote(
        local.at[pl.ds(pl.multiple_of((1 - core) * HALF, 8), HALF), :], core_recv, core_sem.at[0], core_sem.at[1], partner
    )
    give.start()
    lax.fori_loop(3, NF, project, 0)

    for t in range(3):
        load_sound(t).wait()
    slot = lanes((32, 128)) // 8

    def pack_x(f, _):
        for side, tile in ((0, 0), (1, 2)):
            acc = None
            for i in range(16):
                cells = big[f, i // 2, tile, TOP + 32 * (i % 2) : TOP + 32 * (i % 2) + 32, :]
                shift = (8 * (i + side)) % 128
                cells = pltpu.roll(cells, shift, 1) if shift else cells
                acc = cells if acc is None else jnp.where(slot == i, cells, acc)
            xs[side, f] = acc
        return 0

    lax.fori_loop(0, 6, pack_x, 0)
    give.wait()
    half[...] = local[pl.ds(pl.multiple_of(core * HALF, 8), HALF), :] + core_recv[...]

    def scatter(d):
        x, y = plane(d)
        return remote(
            half.at[pl.ds(pl.multiple_of((y * 4 + x) * CHUNK, 8), CHUNK), :],
            xy_recv.at[d], xy_send.at[d], xy_got.at[d], plane_dev(d),
        )

    for d in far:
        scatter(d).start()

    x_copies = [remote(xs.at[s], xr.at[s], xh_send.at[s], xh_got.at[s], sides[s]) for s in range(2)]
    for copy in x_copies:
        copy.start()

    low_rows = lax.broadcasted_iota(jnp.int32, (3, 8, 128), 1) < 4

    def pack_y(l, _):
        for s, r in ((0, TOP), (1, BOT - 8)):
            def strip(f):
                return big[f, l, 0:3, r : r + 8, :]

            def joined(a, b):
                if s == 0:
                    return jnp.where(low_rows, strip(a), pltpu.roll(strip(b), 4, 1))
                return jnp.where(low_rows, pltpu.roll(strip(a), 4, 1), strip(b))

            ys[s, l, 0] = strip(PR)
            ys[s, l, 1] = strip(V)
            ys[s, l, 2] = joined(U, W)
            ys[s, l, 3] = joined(TH, SS)
        return 0

    lax.fori_loop(0, NL, pack_y, 0)
    y_copies = [remote(ys.at[s], yr.at[s], yh_send.at[s], yh_got.at[s], rows_to[s]) for s in range(2)]
    for copy in y_copies:
        copy.start()

    lane4 = lanes((4, 16, 128))
    at_end, at_start = lane4 == 127, lane4 == 0

    def across_x(c):
        fwd, back = pltpu.roll(c, 127, 2), pltpu.roll(c, 1, 2)
        fwd = jnp.where(at_end, jnp.concatenate([fwd[1:], fwd[:1]], axis=0), fwd)
        back = jnp.where(at_start, jnp.concatenate([back[3:], back[:3]], axis=0), back)
        return fwd - back

    def get(f, l, r):
        return big[f, l, :, r : r + 16, :]

    def vertical(f, l, r):
        up = get(f, jnp.minimum(l + 1, NL - 1), r) * jnp.where(l < NL - 1, 1.0, 0.0)
        down = get(f, jnp.maximum(l - 1, 0), r) * jnp.where(l > 0, 1.0, 0.0)
        return up - down

    def winds(rows):
        def body(l, _):
            for r in rows:
                ok = mask[:, r : r + 16, :]
                big[U, l, :, r : r + 16, :] = (get(U, l, r) - 0.25 * across_x(get(PR, l, r))) * ok
                along = get(PR, l, r + 1) - get(PR, l, r - 1)
                big[V, l, :, r : r + 16, :] = (get(V, l, r) - 0.25 * along) * ok
                big[W, l, :, r : r + 16, :] = get(W, l, r) - 0.25 * vertical(PR, l, r) + 0.5 * get(TH, l, r)
            return 0

        lax.fori_loop(0, NL, body, 0)

    def pressure(rows, last=False):
        def body(l, _):
            for r in rows:
                along = get(V, l, r + 1) - get(V, l, r - 1)
                diverge = across_x(get(U, l, r)) + along + vertical(W, l, r)
                new_p = get(PR, l, r) - 0.25 * get(SS, l, r) * diverge
                new_t = get(TH, l, r) - 0.5 * get(W, l, r)
                if last:
                    done = (get(U, l, r), get(V, l, r), get(W, l, r), new_p, new_t)
                    for f, cells in enumerate(done):
                        for t in range(3):
                            adv[f, l, r - TOP : r - TOP + 16, t * 128 : t * 128 + 128] = cells[t]
                else:
                    big[PR, l, :, r : r + 16, :] = new_p * mask[:, r : r + 16, :]
                    big[TH, l, :, r : r + 16, :] = new_t
            return 0

        lax.fori_loop(0, NL, body, 0)

    for d in far:
        scatter(d).wait_recv()
    total = half[pl.ds(pl.multiple_of(me * CHUNK, 8), CHUNK), :]
    for d in range(1, 16):
        total = total + xy_recv[d]
    red[...] = total

    def across(d):
        return remote(red, z_recv.at[d], z_send.at[d], z_got.at[d], column_dev(d))

    for d in deep:
        across(d).start()

    for copy in x_copies:
        copy.wait()
    near = lanes((32, 128)) < 64

    def unpack_x(f, _):
        for i in range(16):
            shift_a, shift_b = (128 - 8 * i) % 128, (128 - 8 * (i + 1)) % 128
            a, b = xr[0, f], xr[1, f]
            a = pltpu.roll(a, shift_a, 1) if shift_a else a
            b = pltpu.roll(b, shift_b, 1) if shift_b else b
            r = TOP + 32 * (i % 2)
            big[f, i // 2, 3, r : r + 32, :] = jnp.where(near, a, b)
        return 0

    lax.fori_loop(0, 6, unpack_x, 0)

    slot8 = lanes((8, 128)) // 16

    def pack_c(f, _):
        for s, r in ((0, TOP), (1, BOT - 8)):
            acc = None
            for l in range(NL):
                shift = (8 + 16 * l) % 128
                cells = pltpu.roll(big[f, l, 3, r : r + 8, :], shift, 1)
                acc = cells if acc is None else jnp.where(slot8 == l, cells, acc)
            cs[s, f] = acc
        return 0

    lax.fori_loop(0, 6, pack_c, 0)
    c_copies = [remote(cs.at[s], cr.at[s], ch_send.at[s], ch_got.at[s], rows_to[s]) for s in range(2)]
    for copy in c_copies:
        copy.start()

    def mask_p(l, _):
        big[PR, l, 3, TOP:BOT, :] = big[PR, l, 3, TOP:BOT, :] * mask[3, TOP:BOT, :]
        return 0

    lax.fori_loop(0, NL, mask_p, 0)
    winds((24, 40, 56))
    for d in deep:
        across(d).wait_recv()
    total = red[...]
    for d in range(1, 8):
        total = total + z_recv[d]

    def chunk_of(q):
        return modes.at[pl.ds(pl.multiple_of(core * HALF + q * CHUNK, 8), CHUNK), :]

    modes[pl.ds(pl.multiple_of(core * HALF + me * CHUNK, 8), CHUNK), :] = total

    def gather(d):
        return remote(chunk_of(me), chunk_of(me), ag_send.at[d], ag_got.at[d], plane_dev(d))

    def forward(d):
        x, y = (px + 4 - d % 4) % 4, (py + 4 - d // 4) % 4
        ref = chunk_of(y * 4 + x)
        return remote(ref, ref, fw_send.at[d], fw_got.at[d], partner)

    for d in far:
        gather(d).start()
    forward(0).start()

    for copy in y_copies:
        copy.wait()
    for copy in c_copies:
        copy.wait()

    def unpack_y(l, _):
        for s, r in ((0, BOT), (1, TOP - 8)):
            def put(f, cells):
                big[f, l, 0:3, r : r + 8, :] = cells

            def other(cells):
                return pltpu.roll(cells, 4, 1)

            put(PR, yr[s, l, 0] * mask[0:3, r : r + 8, :])
            put(V, yr[s, l, 1])
            one, two = yr[s, l, 2], yr[s, l, 3]
            if s == 0:
                put(U, one)
                put(W, other(one))
                put(TH, two)
                put(SS, other(two))
            else:
                put(U, other(one))
                put(W, one)
                put(TH, other(two))
                put(SS, two)
        return 0

    lax.fori_loop(0, NL, unpack_y, 0)

    def unpack_c(f, _):
        for s, r in ((0, BOT), (1, TOP - 8)):
            for l in range(NL):
                big[f, l, 3, r : r + 8, :] = pltpu.roll(cr[s, f], (128 - 8 - 16 * l) % 128, 1)
        return 0

    lax.fori_loop(0, 6, unpack_c, 0)

    def mask_c(l, _):
        for r in (TOP - 8, BOT):
            big[PR, l, 3, r : r + 8, :] = big[PR, l, 3, r : r + 8, :] * mask[3, r : r + 8, :]
        return 0

    lax.fori_loop(0, NL, mask_c, 0)

    every = range(8, 88, 16)
    winds((8, 72))
    pressure(every)
    winds(every)
    pressure(every)
    winds(every)
    for d in far:
        gather(d).wait_recv()
        forward(d).start()
    pressure(range(TOP, BOT, 16), last=True)

    for d in range(16):
        forward(d).wait()
    for d in far:
        scatter(d).wait_send()
        gather(d).wait_send()
    for d in deep:
        across(d).wait_send()


def sum_modes(state, driving, sound, tab_x, tab_y):
    vmem = pl.BlockSpec(memory_space=pltpu.VMEM)
    hbm = pl.BlockSpec(memory_space=pltpu.HBM)
    dma = pltpu.SemaphoreType.DMA
    return pl.pallas_call(
        mode_kernel,
        out_shape=(
            jax.ShapeDtypeStruct((2 * HALF, 128), F32),
            jax.ShapeDtypeStruct((NF, NL, ROWS, COLS), F32),
            jax.ShapeDtypeStruct((384, COLS), BF16),
            jax.ShapeDtypeStruct((64, 256), BF16),
        ),
        in_specs=[hbm] * 5,
        out_specs=(vmem, vmem, vmem, vmem),
        scratch_shapes=[
            pltpu.VMEM((6, NL, 4, 96, 128), F32),
            pltpu.VMEM((NF, NL, ROWS, COLS), F32),
            pltpu.VMEM((MODES, COLS), F32),
            pltpu.VMEM((64, 128), F32),
            pltpu.VMEM((256, COLS), BF16),
            pltpu.VMEM((64, 256), BF16),
            pltpu.VMEM((4, 96, 128), F32),
            pltpu.VMEM((2 * HALF, 128), F32),
            pltpu.VMEM((HALF, 128), F32),
            pltpu.VMEM((HALF, 128), F32),
            pltpu.VMEM((16, CHUNK, 128), F32),
            pltpu.VMEM((CHUNK, 128), F32),
            pltpu.VMEM((8, CHUNK, 128), F32),
            pltpu.VMEM((2, 6, 32, 128), F32),
            pltpu.VMEM((2, 6, 32, 128), F32),
            pltpu.VMEM((2, NL, 4, 3, 8, 128), F32),
            pltpu.VMEM((2, NL, 4, 3, 8, 128), F32),
            pltpu.VMEM((2, 6, 8, 128), F32),
            pltpu.VMEM((2, 6, 8, 128), F32),
            dma((NF, 3)), dma((NF,)), dma((3,)), dma((2,)), dma((2,)),
            dma((16,)), dma((16,)), dma((8,)), dma((8,)),
            dma((16,)), dma((16,)), dma((16,)), dma((16,)),
            dma((2,)), dma((2,)), dma((2,)), dma((2,)), dma((2,)), dma((2,)),
        ],
        compiler_params=pltpu.CompilerParams(
            collective_id=0, has_side_effects=True, vmem_limit_bytes=40 * 1024 * 1024
        ),
        name="sum_modes",
    )(*(pltpu.with_memory_space_constraint(a, pltpu.HBM) for a in (state, driving, sound, tab_x, tab_y)))


def back_kernel(rate, modes, xt3, yt3, adv, out):
    f = pl.program_id(0)
    side = lanes((64, 128)) < 64
    scaled = [modes[q] * jnp.where(side, rate[f, 2 * q], rate[f, 2 * q + 1]) for q in range(4)]
    high, low = split(jnp.concatenate(scaled, axis=1))
    back = dot(yt3[...], jnp.concatenate([high, high, low, low], axis=0))
    rows = []
    for q in range(4):
        both = back[:, 128 * q : 128 * q + 128]
        rows += [jnp.where(side, both, 0.0), jnp.where(side, 0.0, both)]
    high, low = split(jnp.concatenate(rows, axis=0))
    tendency = dot(jnp.concatenate([high, low, high], axis=1), xt3[...])
    out[0] = adv[0] - tendency.reshape(NL, ROWS, COLS)


def nudge(rate, modes, xt3, yt3, adv):
    block = pl.BlockSpec((1, NL, ROWS, COLS), lambda f: (f, 0, 0, 0))
    vmem = pl.BlockSpec(memory_space=pltpu.VMEM)
    return pl.pallas_call(
        back_kernel,
        grid=(NF,),
        out_shape=jax.ShapeDtypeStruct((NF, NL, ROWS, COLS), F32),
        in_specs=[
            pl.BlockSpec(memory_space=pltpu.SMEM),
            pl.BlockSpec((4, 64, 128), lambda f: (f, 0, 0)),
            vmem,
            vmem,
            block,
        ],
        out_specs=block,
        compiler_params=pltpu.CompilerParams(
            dimension_semantics=("arbitrary",), vmem_limit_bytes=24 * 1024 * 1024
        ),
        name="nudge",
    )(rate, modes, xt3, yt3, adv)


def solution(mesh):
    tab_x, tab_y = tables()

    def on_device(state, driving, rate, sound_square):
        modes, adv, xt3, yt3 = sum_modes(state, driving, sound_square, jnp.asarray(tab_x), jnp.asarray(tab_y))
        return nudge(rate, modes.reshape(20, 64, 128), xt3, yt3, adv)

    return jax.shard_map(
        on_device,
        mesh=mesh,
        in_specs=(P(None, None, "gy", "gx"), P(None, None, "gy", "gx"), P(), P(None, "gy", "gx")),
        out_specs=P(None, None, "gy", "gx"),
        check_vma=False,
    )
```

```python
import jax
import jax.numpy as jnp
import numpy as np
from jax import lax
from jax.experimental import pallas as pl
from jax.experimental.pallas import tpu as pltpu
from jax.sharding import PartitionSpec as P

MODES = 64
SUBSTEPS = 3
NX = 3072
NY = 2048
NF, NL, ROWS, COLS = 5, 8, 64, 384
GX, GY = 8, 32
F32, BF16 = jnp.float32, jnp.bfloat16
MESH = pl.DeviceIdType.MESH
TOP, BOT = 16, 80
HALF, CHUNK = 640, 40
UNROLL = 2
U, V, W, PR, TH, SS = range(6)


def basis(size):
    index = np.arange(size, dtype=np.int64)
    order = np.arange(MODES, dtype=np.int64)
    freq = np.where(order < MODES // 2, order, order - MODES // 2 + 1)
    wrapped = (freq[:, None] * (2 * index[None, :] + 1)) % (2 * size)
    phase = np.float32(np.pi) * wrapped.astype(np.float32) / np.float32(size)
    phase = phase.astype(np.float64)
    table = np.where(order[:, None] < MODES // 2, np.cos(phase), np.sin(phase))
    scaling = np.where(order == 0, 1.0 / size, 2.0 / size).astype(np.float32)
    table = table.astype(np.float32)
    return table, table * scaling[:, None]


def tables():
    basis_x, _ = basis(NX)
    basis_y, weight_y = basis(NY)
    tab_x = basis_x.reshape(MODES, GX, COLS).transpose(1, 0, 2)
    by_tile = basis_y.reshape(MODES, GY, ROWS).transpose(1, 2, 0)
    wy_tile = weight_y.reshape(MODES, GY, ROWS).transpose(1, 0, 2)
    return np.ascontiguousarray(tab_x), np.concatenate([wy_tile, by_tile], axis=2)


def lanes(shape):
    return lax.broadcasted_iota(jnp.int32, shape, len(shape) - 1)


def split(x):
    high = x.astype(BF16)
    return high, (x - high.astype(F32)).astype(BF16)


def y_table(pair):
    lane = lanes(pair.shape)
    high = pair.astype(BF16).astype(F32)
    first = jnp.where(lane < 64, high, pair - high)
    second = jnp.where(lane < 64, high, 0.0)
    return jnp.concatenate([first, second], axis=1).astype(BF16)


def dot(a, b):
    return jnp.dot(a, b, preferred_element_type=F32)


def mode_kernel(
    state, driving, sound, tab_x, tab_y,
    modes, adv, xt3, yt3,
    big, drv, tx, ty, wx, wy, mask, local, half, core_recv, xy_recv, red, z_recv,
    xs, xr, ys, yr, cs, cr,
    ld_sem, drv_sem, snd_sem, tab_sem, core_sem, xy_send, xy_got, z_send, z_got,
    ag_send, ag_got, fw_send, fw_got, xh_send, xh_got, yh_send, yh_got, ch_send, ch_got,
):
    gx, gy = lax.axis_index("gx"), lax.axis_index("gy")
    py, zlo = gx // 2, gx % 2
    core, px, zhi = gy % 2, (gy // 2) % 4, gy // 8
    pz = zhi * 2 + zlo
    me = py * 4 + px

    def at(x, y, z, c):
        return {"gx": y * 2 + z % 2, "gy": ((z // 2) * 4 + x) * 2 + c}

    partner = at(px, py, pz, 1 - core)

    def plane(d):
        return (px + d % 4) % 4, (py + d // 4) % 4

    def plane_dev(d):
        x, y = plane(d)
        return at(x, y, pz, core)

    def column_dev(d):
        return at(px, py, (pz + d) % 8, core)

    left, right = {"gx": (gx + GX - 1) % GX, "gy": gy}, {"gx": (gx + 1) % GX, "gy": gy}
    above, below = {"gx": gx, "gy": (gy + GY - 1) % GY}, {"gx": gx, "gy": (gy + 1) % GY}
    sides = (left, right)
    rows_to = (above, below)

    far = sorted(range(1, 16), key=lambda d: -(min(d % 4, 4 - d % 4) + min(d // 4, 4 - d // 4)))
    deep = sorted(range(1, 8), key=lambda d: -min(d, 8 - d))

    barrier = pltpu.get_barrier_semaphore()
    peers = [partner] + [plane_dev(d) for d in far] + [column_dev(d) for d in deep]
    peers += [left, right, above, below]
    for peer in peers:
        pl.semaphore_signal(barrier, inc=1, device_id=peer, device_id_type=MESH)

    def remote(src, dst, send, recv, dev):
        return pltpu.make_async_remote_copy(
            src_ref=src, dst_ref=dst, send_sem=send, recv_sem=recv, device_id=dev, device_id_type=MESH
        )

    def load(f, t):
        return pltpu.make_async_copy(
            state.at[f, :, :, pl.ds(t * 128, 128)], big.at[f, :, t, pl.ds(TOP, ROWS), :], ld_sem.at[f, t]
        )

    def load_drv(f):
        return pltpu.make_async_copy(driving.at[f], drv.at[f], drv_sem.at[f])

    def load_sound(t):
        return pltpu.make_async_copy(
            sound.at[:, :, pl.ds(t * 128, 128)], big.at[SS, :, t, pl.ds(TOP, ROWS), :], snd_sem.at[t]
        )

    get_tx = pltpu.make_async_copy(tab_x.at[gx], tx, tab_sem.at[0])
    get_ty = pltpu.make_async_copy(tab_y.at[gy], ty, tab_sem.at[1])
    get_tx.start()
    get_ty.start()
    def nth(i):
        return jnp.where(core == 0, NF - 1 - i, i)

    for i in range(NF):
        for t in range(3):
            load(nth(i), t).start()
        load_drv(nth(i)).start()
    for t in range(3):
        load_sound(t).start()

    get_tx.wait()
    get_ty.wait()
    b_x = tx[...]
    k_row = lax.broadcasted_iota(jnp.int32, b_x.shape, 0)
    w_x = b_x * jnp.where(k_row == 0, np.float32(1.0 / NX), np.float32(2.0 / NX))
    w_hi, w_lo = split(w_x)
    wx[...] = jnp.concatenate([w_hi, w_hi, w_lo, w_lo], axis=0)
    b_hi, b_lo = split(b_x)
    xt3[...] = jnp.concatenate([b_hi, b_hi, b_hi, b_hi, b_lo, b_lo], axis=0)
    pair = ty[...]
    lane2 = lanes(pair.shape)
    turned = pltpu.roll(pair, 64, 1)
    wy[...] = y_table(jnp.where(lane2 < 64, pair, turned))
    yt3[...] = y_table(jnp.where(lane2 < 64, turned, pair))

    row = lax.broadcasted_iota(jnp.int32, (96, 128), 0)
    lane = lanes((96, 128))
    row_ok = ((row >= TOP) | (gy > 0)) & ((row < BOT) | (gy < GY - 1))
    col_ok = jnp.where(lane < 64, jnp.where(gx < GX - 1, 1.0, 0.0), jnp.where(gx > 0, 1.0, 0.0))
    row_ok = jnp.where(row_ok, 1.0, 0.0)
    for t in range(3):
        mask[t] = row_ok
    mask[3] = row_ok * col_ok

    def project(i, _):
        f = nth(i)
        for t in range(3):
            load(f, t).wait()
        load_drv(f).wait()
        diff = jnp.concatenate(
            [
                big[f, :, t, TOP:BOT, :].reshape(512, 128)
                - drv[f, :, :, t * 128 : (t + 1) * 128].reshape(512, 128)
                for t in range(3)
            ],
            axis=1,
        )
        high, low = split(diff)
        nt = (((1,), (1,)), ((), ()))
        a = lax.dot_general(high, wx[...], nt, preferred_element_type=F32)
        b = lax.dot_general(low, wx[0:128], nt, preferred_element_type=F32)
        part = a[:, :128] + (a[:, 128:] + b)
        side = lanes((64, 128))
        pairs = [
            jnp.where(side < 64, part[128 * q : 128 * q + 64], part[128 * q + 64 : 128 * q + 128])
            for q in range(4)
        ]
        high, low = split(jnp.concatenate(pairs, axis=1))
        rhs = jnp.concatenate([high, high, low, low], axis=0)
        out = dot(wy[...], rhs)
        for q in range(4):
            local[pl.ds(pl.multiple_of((f * 4 + q) * 64, 64), 64), :] = out[:, 128 * q : 128 * q + 128]
        return 0

    lax.fori_loop(0, 3, project, 0)
    pl.semaphore_wait(barrier, len(peers))

    give = remote(
        local.at[pl.ds(pl.multiple_of((1 - core) * HALF, 8), HALF), :], core_recv, core_sem.at[0], core_sem.at[1], partner
    )
    give.start()
    lax.fori_loop(3, NF, project, 0)

    for t in range(3):
        load_sound(t).wait()
    slot = lanes((32, 128)) // 8

    def pack_x(f, _):
        for side, tile in ((0, 0), (1, 2)):
            acc = None
            for i in range(16):
                cells = big[f, i // 2, tile, TOP + 32 * (i % 2) : TOP + 32 * (i % 2) + 32, :]
                shift = (8 * (i + side)) % 128
                cells = pltpu.roll(cells, shift, 1) if shift else cells
                acc = cells if acc is None else jnp.where(slot == i, cells, acc)
            xs[side, f] = acc
        return 0

    lax.fori_loop(0, 6, pack_x, 0)
    low_rows = lax.broadcasted_iota(jnp.int32, (3, 8, 128), 1) < 4

    def pack_y(l, _):
        for s, r in ((0, TOP), (1, BOT - 8)):
            def strip(f):
                return big[f, l, 0:3, r : r + 8, :]

            def joined(a, b):
                if s == 0:
                    return jnp.where(low_rows, strip(a), pltpu.roll(strip(b), 4, 1))
                return jnp.where(low_rows, pltpu.roll(strip(a), 4, 1), strip(b))

            ys[s, l, 0] = strip(PR)
            ys[s, l, 1] = strip(V)
            ys[s, l, 2] = joined(U, W)
            ys[s, l, 3] = joined(TH, SS)
        return 0

    lax.fori_loop(0, NL, pack_y, 0)
    give.wait()
    half[...] = local[pl.ds(pl.multiple_of(core * HALF, 8), HALF), :] + core_recv[...]

    def scatter(d):
        x, y = plane(d)
        return remote(
            half.at[pl.ds(pl.multiple_of((y * 4 + x) * CHUNK, 8), CHUNK), :],
            xy_recv.at[d], xy_send.at[d], xy_got.at[d], plane_dev(d),
        )

    for d in far:
        scatter(d).start()

    y_copies = [remote(ys.at[s], yr.at[s], yh_send.at[s], yh_got.at[s], rows_to[s]) for s in range(2)]
    for copy in y_copies:
        copy.start()

    x_copies = [remote(xs.at[s], xr.at[s], xh_send.at[s], xh_got.at[s], sides[s]) for s in range(2)]
    for copy in x_copies:
        copy.start()

    lane4 = lanes((4, 16, 128))
    at_end, at_start = lane4 == 127, lane4 == 0

    def across_x(c):
        fwd, back = pltpu.roll(c, 127, 2), pltpu.roll(c, 1, 2)
        fwd = jnp.where(at_end, jnp.concatenate([fwd[1:], fwd[:1]], axis=0), fwd)
        back = jnp.where(at_start, jnp.concatenate([back[3:], back[:3]], axis=0), back)
        return fwd - back

    def get(f, l, r):
        return big[f, l, :, r : r + 16, :]

    def vertical(f, l, r):
        up = get(f, jnp.minimum(l + 1, NL - 1), r) * jnp.where(l < NL - 1, 1.0, 0.0)
        down = get(f, jnp.maximum(l - 1, 0), r) * jnp.where(l > 0, 1.0, 0.0)
        return up - down

    def winds(rows):
        def body(l, _):
            for r in rows:
                ok = mask[:, r : r + 16, :]
                big[U, l, :, r : r + 16, :] = (get(U, l, r) - 0.25 * across_x(get(PR, l, r))) * ok
                along = get(PR, l, r + 1) - get(PR, l, r - 1)
                big[V, l, :, r : r + 16, :] = (get(V, l, r) - 0.25 * along) * ok
                big[W, l, :, r : r + 16, :] = get(W, l, r) - 0.25 * vertical(PR, l, r) + 0.5 * get(TH, l, r)
            return 0

        lax.fori_loop(0, NL, body, 0, unroll=UNROLL)

    def pressure(rows, last=False):
        def body(l, _):
            for r in rows:
                along = get(V, l, r + 1) - get(V, l, r - 1)
                diverge = across_x(get(U, l, r)) + along + vertical(W, l, r)
                new_p = get(PR, l, r) - 0.25 * get(SS, l, r) * diverge
                new_t = get(TH, l, r) - 0.5 * get(W, l, r)
                if last:
                    done = (get(U, l, r), get(V, l, r), get(W, l, r), new_p, new_t)
                    for f, cells in enumerate(done):
                        for t in range(3):
                            adv[f, l, r - TOP : r - TOP + 16, t * 128 : t * 128 + 128] = cells[t]
                else:
                    big[PR, l, :, r : r + 16, :] = new_p * mask[:, r : r + 16, :]
                    big[TH, l, :, r : r + 16, :] = new_t
            return 0

        lax.fori_loop(0, NL, body, 0, unroll=UNROLL)

    for d in far:
        scatter(d).wait_recv()
    total = half[pl.ds(pl.multiple_of(me * CHUNK, 8), CHUNK), :]
    for d in range(1, 16):
        total = total + xy_recv[d]
    red[...] = total

    def across(d):
        return remote(red, z_recv.at[d], z_send.at[d], z_got.at[d], column_dev(d))

    for d in deep:
        across(d).start()

    for copy in x_copies:
        copy.wait()
    near = lanes((32, 128)) < 64

    def unpack_x(f, _):
        for i in range(16):
            shift_a, shift_b = (128 - 8 * i) % 128, (128 - 8 * (i + 1)) % 128
            a, b = xr[0, f], xr[1, f]
            a = pltpu.roll(a, shift_a, 1) if shift_a else a
            b = pltpu.roll(b, shift_b, 1) if shift_b else b
            r = TOP + 32 * (i % 2)
            big[f, i // 2, 3, r : r + 32, :] = jnp.where(near, a, b)
        return 0

    lax.fori_loop(0, 6, unpack_x, 0)

    slot8 = lanes((8, 128)) // 16

    def pack_c(f, _):
        for s, r in ((0, TOP), (1, BOT - 8)):
            acc = None
            for l in range(NL):
                shift = (8 + 16 * l) % 128
                cells = pltpu.roll(big[f, l, 3, r : r + 8, :], shift, 1)
                acc = cells if acc is None else jnp.where(slot8 == l, cells, acc)
            cs[s, f] = acc
        return 0

    lax.fori_loop(0, 6, pack_c, 0)
    c_copies = [remote(cs.at[s], cr.at[s], ch_send.at[s], ch_got.at[s], rows_to[s]) for s in range(2)]
    for copy in c_copies:
        copy.start()

    def mask_p(l, _):
        big[PR, l, 3, TOP:BOT, :] = big[PR, l, 3, TOP:BOT, :] * mask[3, TOP:BOT, :]
        return 0

    lax.fori_loop(0, NL, mask_p, 0)
    winds((24, 40, 56))
    for d in deep:
        across(d).wait_recv()
    total = red[...]
    for d in range(1, 8):
        total = total + z_recv[d]

    def chunk_of(q):
        return modes.at[pl.ds(pl.multiple_of(core * HALF + q * CHUNK, 8), CHUNK), :]

    modes[pl.ds(pl.multiple_of(core * HALF + me * CHUNK, 8), CHUNK), :] = total

    def gather(d):
        return remote(chunk_of(me), chunk_of(me), ag_send.at[d], ag_got.at[d], plane_dev(d))

    def forward(d):
        x, y = (px + 4 - d % 4) % 4, (py + 4 - d // 4) % 4
        ref = chunk_of(y * 4 + x)
        return remote(ref, ref, fw_send.at[d], fw_got.at[d], partner)

    for d in far:
        gather(d).start()
    forward(0).start()

    for copy in y_copies:
        copy.wait()
    for copy in c_copies:
        copy.wait()

    def unpack_y(l, _):
        for s, r in ((0, BOT), (1, TOP - 8)):
            def put(f, cells):
                big[f, l, 0:3, r : r + 8, :] = cells

            def other(cells):
                return pltpu.roll(cells, 4, 1)

            put(PR, yr[s, l, 0] * mask[0:3, r : r + 8, :])
            put(V, yr[s, l, 1])
            one, two = yr[s, l, 2], yr[s, l, 3]
            if s == 0:
                put(U, one)
                put(W, other(one))
                put(TH, two)
                put(SS, other(two))
            else:
                put(U, other(one))
                put(W, one)
                put(TH, other(two))
                put(SS, two)
        return 0

    lax.fori_loop(0, NL, unpack_y, 0)

    def unpack_c(f, _):
        for s, r in ((0, BOT), (1, TOP - 8)):
            for l in range(NL):
                big[f, l, 3, r : r + 8, :] = pltpu.roll(cr[s, f], (128 - 8 - 16 * l) % 128, 1)
        return 0

    lax.fori_loop(0, 6, unpack_c, 0)

    def mask_c(l, _):
        for r in (TOP - 8, BOT):
            big[PR, l, 3, r : r + 8, :] = big[PR, l, 3, r : r + 8, :] * mask[3, r : r + 8, :]
        return 0

    lax.fori_loop(0, NL, mask_c, 0)

    every = range(8, 88, 16)
    winds((8, 72))
    pressure(every)
    winds(every)
    pressure(every)
    winds(every)
    for d in far:
        gather(d).wait_recv()
        forward(d).start()
    pressure(range(TOP, BOT, 16), last=True)

    for d in range(16):
        forward(d).wait()
    for d in far:
        scatter(d).wait_send()
        gather(d).wait_send()
    for d in deep:
        across(d).wait_send()


def sum_modes(state, driving, sound, tab_x, tab_y):
    vmem = pl.BlockSpec(memory_space=pltpu.VMEM)
    hbm = pl.BlockSpec(memory_space=pltpu.HBM)
    dma = pltpu.SemaphoreType.DMA
    return pl.pallas_call(
        mode_kernel,
        out_shape=(
            jax.ShapeDtypeStruct((2 * HALF, 128), F32),
            jax.ShapeDtypeStruct((NF, NL, ROWS, COLS), F32),
            jax.ShapeDtypeStruct((384, COLS), BF16),
            jax.ShapeDtypeStruct((64, 256), BF16),
        ),
        in_specs=[hbm] * 5,
        out_specs=(vmem, vmem, vmem, vmem),
        scratch_shapes=[
            pltpu.VMEM((6, NL, 4, 96, 128), F32),
            pltpu.VMEM((NF, NL, ROWS, COLS), F32),
            pltpu.VMEM((MODES, COLS), F32),
            pltpu.VMEM((64, 128), F32),
            pltpu.VMEM((256, COLS), BF16),
            pltpu.VMEM((64, 256), BF16),
            pltpu.VMEM((4, 96, 128), F32),
            pltpu.VMEM((2 * HALF, 128), F32),
            pltpu.VMEM((HALF, 128), F32),
            pltpu.VMEM((HALF, 128), F32),
            pltpu.VMEM((16, CHUNK, 128), F32),
            pltpu.VMEM((CHUNK, 128), F32),
            pltpu.VMEM((8, CHUNK, 128), F32),
            pltpu.VMEM((2, 6, 32, 128), F32),
            pltpu.VMEM((2, 6, 32, 128), F32),
            pltpu.VMEM((2, NL, 4, 3, 8, 128), F32),
            pltpu.VMEM((2, NL, 4, 3, 8, 128), F32),
            pltpu.VMEM((2, 6, 8, 128), F32),
            pltpu.VMEM((2, 6, 8, 128), F32),
            dma((NF, 3)), dma((NF,)), dma((3,)), dma((2,)), dma((2,)),
            dma((16,)), dma((16,)), dma((8,)), dma((8,)),
            dma((16,)), dma((16,)), dma((16,)), dma((16,)),
            dma((2,)), dma((2,)), dma((2,)), dma((2,)), dma((2,)), dma((2,)),
        ],
        compiler_params=pltpu.CompilerParams(
            collective_id=0, has_side_effects=True, vmem_limit_bytes=40 * 1024 * 1024
        ),
        name="sum_modes",
    )(*(pltpu.with_memory_space_constraint(a, pltpu.HBM) for a in (state, driving, sound, tab_x, tab_y)))


def back_kernel(rate, modes, xt3, yt3, adv, out, held, done, sem):
    side = lanes((64, 128)) < 64
    for f in range(NF):
        scaled = [
            modes[4 * f + q] * jnp.where(side, rate[f, 2 * q], rate[f, 2 * q + 1]) for q in range(4)
        ]
        high, low = split(jnp.concatenate(scaled, axis=1))
        held[f] = dot(yt3[...], jnp.concatenate([high, high, low, low], axis=0))

    def write(f):
        return pltpu.make_async_copy(done.at[f], out.at[f], sem.at[f])

    for f in range(NF):
        rows = []
        for q in range(4):
            both = held[f, :, 128 * q : 128 * q + 128]
            rows += [jnp.where(side, both, 0.0), jnp.where(side, 0.0, both)]
        high, low = split(jnp.concatenate(rows, axis=0))
        tendency = dot(jnp.concatenate([high, low, high], axis=1), xt3[...])
        done[f] = adv[f] - tendency.reshape(NL, ROWS, COLS)
        write(f).start()
    for f in range(NF):
        write(f).wait()


def nudge(rate, modes, xt3, yt3, adv):
    vmem = pl.BlockSpec(memory_space=pltpu.VMEM)
    return pl.pallas_call(
        back_kernel,
        out_shape=jax.ShapeDtypeStruct((NF, NL, ROWS, COLS), F32),
        in_specs=[pl.BlockSpec(memory_space=pltpu.SMEM)] + [vmem] * 4,
        out_specs=pl.BlockSpec(memory_space=pltpu.HBM),
        scratch_shapes=[
            pltpu.VMEM((NF, 64, 512), F32),
            pltpu.VMEM((NF, NL, ROWS, COLS), F32),
            pltpu.SemaphoreType.DMA((NF,)),
        ],
        compiler_params=pltpu.CompilerParams(vmem_limit_bytes=32 * 1024 * 1024),
        name="nudge",
    )(rate, modes, xt3, yt3, adv)


def solution(mesh):
    tab_x, tab_y = tables()

    def on_device(state, driving, rate, sound_square):
        modes, adv, xt3, yt3 = sum_modes(state, driving, sound_square, jnp.asarray(tab_x), jnp.asarray(tab_y))
        return nudge(rate, modes.reshape(20, 64, 128), xt3, yt3, adv)

    return jax.shard_map(
        on_device,
        mesh=mesh,
        in_specs=(P(None, None, "gy", "gx"), P(None, None, "gy", "gx"), P(), P(None, "gy", "gx")),
        out_specs=P(None, None, "gy", "gx"),
        check_vma=False,
    )
```

```python
import jax
import jax.numpy as jnp
import numpy as np
from jax import lax
from jax.experimental import pallas as pl
from jax.experimental.pallas import tpu as pltpu
from jax.sharding import PartitionSpec as P

MODES = 64
SUBSTEPS = 3
NX = 3072
NY = 2048
NF, NL, ROWS, COLS = 5, 8, 64, 384
GX, GY = 8, 32
F32, BF16 = jnp.float32, jnp.bfloat16
MESH = pl.DeviceIdType.MESH
TOP, BOT = 16, 80
HALF, CHUNK = 640, 40
UNROLL = 2
U, V, W, PR, TH, SS = range(6)


def basis(size):
    index = np.arange(size, dtype=np.int64)
    order = np.arange(MODES, dtype=np.int64)
    freq = np.where(order < MODES // 2, order, order - MODES // 2 + 1)
    wrapped = (freq[:, None] * (2 * index[None, :] + 1)) % (2 * size)
    phase = np.float32(np.pi) * wrapped.astype(np.float32) / np.float32(size)
    phase = phase.astype(np.float64)
    table = np.where(order[:, None] < MODES // 2, np.cos(phase), np.sin(phase))
    scaling = np.where(order == 0, 1.0 / size, 2.0 / size).astype(np.float32)
    table = table.astype(np.float32)
    return table, table * scaling[:, None]


def tables():
    basis_x, _ = basis(NX)
    basis_y, weight_y = basis(NY)
    tab_x = basis_x.reshape(MODES, GX, COLS).transpose(1, 0, 2)
    by_tile = basis_y.reshape(MODES, GY, ROWS).transpose(1, 2, 0)
    wy_tile = weight_y.reshape(MODES, GY, ROWS).transpose(1, 0, 2)
    return np.ascontiguousarray(tab_x), np.concatenate([wy_tile, by_tile], axis=2)


def lanes(shape):
    return lax.broadcasted_iota(jnp.int32, shape, len(shape) - 1)


def split(x):
    high = x.astype(BF16)
    return high, (x - high.astype(F32)).astype(BF16)


def y_table(pair):
    lane = lanes(pair.shape)
    high = pair.astype(BF16).astype(F32)
    first = jnp.where(lane < 64, high, pair - high)
    second = jnp.where(lane < 64, high, 0.0)
    return jnp.concatenate([first, second], axis=1).astype(BF16)


def dot(a, b):
    return jnp.dot(a, b, preferred_element_type=F32)


def mode_kernel(
    state, driving, sound, tab_x, tab_y,
    modes, adv, xt3, yt3,
    big, drv, tx, ty, wx, wy, mask, local, half, core_recv, xy_recv, red, z_recv,
    xs, xr, ys, yr, cs, cr,
    ld_sem, drv_sem, snd_sem, tab_sem, core_sem, xy_send, xy_got, z_send, z_got,
    ag_send, ag_got, fw_send, fw_got, xh_send, xh_got, yh_send, yh_got, ch_send, ch_got,
):
    gx, gy = lax.axis_index("gx"), lax.axis_index("gy")
    py, zlo = gx // 2, gx % 2
    core, px, zhi = gy % 2, (gy // 2) % 4, gy // 8
    pz = zhi * 2 + zlo
    me = py * 4 + px

    def at(x, y, z, c):
        return {"gx": y * 2 + z % 2, "gy": ((z // 2) * 4 + x) * 2 + c}

    partner = at(px, py, pz, 1 - core)

    def plane(d):
        return (px + d % 4) % 4, (py + d // 4) % 4

    def plane_dev(d):
        x, y = plane(d)
        return at(x, y, pz, core)

    def column_dev(d):
        return at(px, py, (pz + d) % 8, core)

    left, right = {"gx": (gx + GX - 1) % GX, "gy": gy}, {"gx": (gx + 1) % GX, "gy": gy}
    above, below = {"gx": gx, "gy": (gy + GY - 1) % GY}, {"gx": gx, "gy": (gy + 1) % GY}
    sides = (left, right)
    rows_to = (above, below)

    far = sorted(range(1, 16), key=lambda d: -(min(d % 4, 4 - d % 4) + min(d // 4, 4 - d // 4)))
    deep = sorted(range(1, 8), key=lambda d: -min(d, 8 - d))

    barrier = pltpu.get_barrier_semaphore()
    peers = [partner] + [plane_dev(d) for d in far] + [column_dev(d) for d in deep]
    peers += [left, right, above, below]
    for peer in peers:
        pl.semaphore_signal(barrier, inc=1, device_id=peer, device_id_type=MESH)

    def remote(src, dst, send, recv, dev):
        return pltpu.make_async_remote_copy(
            src_ref=src, dst_ref=dst, send_sem=send, recv_sem=recv, device_id=dev, device_id_type=MESH
        )

    def load(f, t):
        return pltpu.make_async_copy(
            state.at[f, :, :, pl.ds(t * 128, 128)], big.at[f, :, t, pl.ds(TOP, ROWS), :], ld_sem.at[f, t]
        )

    def load_drv(f):
        return pltpu.make_async_copy(driving.at[f], drv.at[f], drv_sem.at[f])

    def load_sound(t):
        return pltpu.make_async_copy(
            sound.at[:, :, pl.ds(t * 128, 128)], big.at[SS, :, t, pl.ds(TOP, ROWS), :], snd_sem.at[t]
        )

    get_tx = pltpu.make_async_copy(tab_x.at[gx], tx, tab_sem.at[0])
    get_ty = pltpu.make_async_copy(tab_y.at[gy], ty, tab_sem.at[1])
    get_tx.start()
    get_ty.start()
    def nth(i):
        return jnp.where(core == 0, NF - 1 - i, i)

    for i in range(NF):
        for t in range(3):
            load(nth(i), t).start()
        load_drv(nth(i)).start()
    for t in range(3):
        load_sound(t).start()

    get_tx.wait()
    get_ty.wait()
    b_x = tx[...]
    k_row = lax.broadcasted_iota(jnp.int32, b_x.shape, 0)
    w_x = b_x * jnp.where(k_row == 0, np.float32(1.0 / NX), np.float32(2.0 / NX))
    w_hi, w_lo = split(w_x)
    wx[...] = jnp.concatenate([w_hi, w_hi, w_lo, w_lo], axis=0)
    b_hi, b_lo = split(b_x)
    xt3[...] = jnp.concatenate([b_hi, b_hi, b_hi, b_hi, b_lo, b_lo], axis=0)
    pair = ty[...]
    lane2 = lanes(pair.shape)
    turned = pltpu.roll(pair, 64, 1)
    wy[...] = y_table(jnp.where(lane2 < 64, pair, turned))
    yt3[...] = y_table(jnp.where(lane2 < 64, turned, pair))

    row = lax.broadcasted_iota(jnp.int32, (96, 128), 0)
    lane = lanes((96, 128))
    row_ok = ((row >= TOP) | (gy > 0)) & ((row < BOT) | (gy < GY - 1))
    col_ok = jnp.where(lane < 64, jnp.where(gx < GX - 1, 1.0, 0.0), jnp.where(gx > 0, 1.0, 0.0))
    row_ok = jnp.where(row_ok, 1.0, 0.0)
    for t in range(3):
        mask[t] = row_ok
    mask[3] = row_ok * col_ok

    def project(i, _):
        f = nth(i)
        for t in range(3):
            load(f, t).wait()
        load_drv(f).wait()
        diff = jnp.concatenate(
            [
                big[f, :, t, TOP:BOT, :].reshape(512, 128)
                - drv[f, :, :, t * 128 : (t + 1) * 128].reshape(512, 128)
                for t in range(3)
            ],
            axis=1,
        )
        high, low = split(diff)
        nt = (((1,), (1,)), ((), ()))
        a = lax.dot_general(high, wx[...], nt, preferred_element_type=F32)
        b = lax.dot_general(low, wx[0:128], nt, preferred_element_type=F32)
        part = a[:, :128] + (a[:, 128:] + b)
        side = lanes((64, 128))
        pairs = [
            jnp.where(side < 64, part[128 * q : 128 * q + 64], part[128 * q + 64 : 128 * q + 128])
            for q in range(4)
        ]
        high, low = split(jnp.concatenate(pairs, axis=1))
        rhs = jnp.concatenate([high, high, low, low], axis=0)
        out = dot(wy[...], rhs)
        for q in range(4):
            local[pl.ds(pl.multiple_of((f * 4 + q) * 64, 64), 64), :] = out[:, 128 * q : 128 * q + 128]
        return 0

    lax.fori_loop(0, 3, project, 0)
    pl.semaphore_wait(barrier, len(peers))

    give = remote(
        local.at[pl.ds(pl.multiple_of((1 - core) * HALF, 8), HALF), :], core_recv, core_sem.at[0], core_sem.at[1], partner
    )
    give.start()
    lax.fori_loop(3, NF, project, 0)

    for t in range(3):
        load_sound(t).wait()
    slot = lanes((32, 128)) // 8

    def pack_x(f, _):
        for side, tile in ((0, 0), (1, 2)):
            acc = None
            for i in range(16):
                cells = big[f, i // 2, tile, TOP + 32 * (i % 2) : TOP + 32 * (i % 2) + 32, :]
                shift = (8 * (i + side)) % 128
                cells = pltpu.roll(cells, shift, 1) if shift else cells
                acc = cells if acc is None else jnp.where(slot == i, cells, acc)
            xs[side, f] = acc
        return 0

    lax.fori_loop(0, 6, pack_x, 0)
    sub = lax.broadcasted_iota(jnp.int32, (3, 8, 128), 1)
    low_rows = sub < 4

    def edge(f, l, r):
        return big[f, l, 0:3, r : r + 8, :]

    def edge_z(l, r):
        up = edge(PR, jnp.minimum(l + 1, NL - 1), r) * jnp.where(l < NL - 1, 1.0, 0.0)
        down = edge(PR, jnp.maximum(l - 1, 0), r) * jnp.where(l > 0, 1.0, 0.0)
        return up - down

    def pack_y(l, _):
        for s, r in ((0, TOP), (1, BOT - 8)):
            def joined(a, b):
                if s == 0:
                    return jnp.where(low_rows, a, pltpu.roll(b, 4, 1))
                return jnp.where(low_rows, pltpu.roll(a, 4, 1), b)

            w_1 = edge(W, l, r) - 0.25 * edge_z(l, r) + 0.5 * edge(TH, l, r)
            t_1 = edge(TH, l, r) - 0.5 * w_1
            v_0 = edge(V, l, r)
            v_1 = v_0 - 0.25 * (edge(PR, l, r + 1) - edge(PR, l, r - 1))
            first = sub == (0 if s == 0 else 7)
            v = jnp.where(first, v_0, v_1)
            ys[s, l, 0] = joined(edge(U, l, r), w_1)
            ys[s, l, 1] = joined(edge(PR, l, r), edge(SS, l, r))
            if s == 0:
                ys[s, l, 2] = jnp.where(sub < 5, v, pltpu.roll(t_1, 5, 1))
            else:
                ys[s, l, 2] = jnp.where(sub >= 3, v, pltpu.roll(t_1, 2, 1))
        return 0

    lax.fori_loop(0, NL, pack_y, 0)
    give.wait()
    half[...] = local[pl.ds(pl.multiple_of(core * HALF, 8), HALF), :] + core_recv[...]

    def scatter(d):
        x, y = plane(d)
        return remote(
            half.at[pl.ds(pl.multiple_of((y * 4 + x) * CHUNK, 8), CHUNK), :],
            xy_recv.at[d], xy_send.at[d], xy_got.at[d], plane_dev(d),
        )

    for d in far:
        scatter(d).start()

    y_copies = [remote(ys.at[s], yr.at[s], yh_send.at[s], yh_got.at[s], rows_to[s]) for s in range(2)]
    for copy in y_copies:
        copy.start()

    x_copies = [remote(xs.at[s], xr.at[s], xh_send.at[s], xh_got.at[s], sides[s]) for s in range(2)]
    for copy in x_copies:
        copy.start()

    lane4 = lanes((4, 16, 128))
    at_end, at_start = lane4 == 127, lane4 == 0

    def across_x(c):
        fwd, back = pltpu.roll(c, 127, 2), pltpu.roll(c, 1, 2)
        fwd = jnp.where(at_end, jnp.concatenate([fwd[1:], fwd[:1]], axis=0), fwd)
        back = jnp.where(at_start, jnp.concatenate([back[3:], back[:3]], axis=0), back)
        return fwd - back

    def get(f, l, r):
        return big[f, l, :, r : r + 16, :]

    def vertical(f, l, r):
        up = get(f, jnp.minimum(l + 1, NL - 1), r) * jnp.where(l < NL - 1, 1.0, 0.0)
        down = get(f, jnp.maximum(l - 1, 0), r) * jnp.where(l > 0, 1.0, 0.0)
        return up - down

    def winds(rows):
        def body(l, _):
            for r in rows:
                ok = mask[:, r : r + 16, :]
                big[U, l, :, r : r + 16, :] = (get(U, l, r) - 0.25 * across_x(get(PR, l, r))) * ok
                along = get(PR, l, r + 1) - get(PR, l, r - 1)
                big[V, l, :, r : r + 16, :] = (get(V, l, r) - 0.25 * along) * ok
                big[W, l, :, r : r + 16, :] = get(W, l, r) - 0.25 * vertical(PR, l, r) + 0.5 * get(TH, l, r)
            return 0

        lax.fori_loop(0, NL, body, 0, unroll=UNROLL)

    def pressure(rows, last=False):
        def body(l, _):
            for r in rows:
                along = get(V, l, r + 1) - get(V, l, r - 1)
                diverge = across_x(get(U, l, r)) + along + vertical(W, l, r)
                new_p = get(PR, l, r) - 0.25 * get(SS, l, r) * diverge
                new_t = get(TH, l, r) - 0.5 * get(W, l, r)
                if last:
                    done = (get(U, l, r), get(V, l, r), get(W, l, r), new_p, new_t)
                    for f, cells in enumerate(done):
                        for t in range(3):
                            adv[f, l, r - TOP : r - TOP + 16, t * 128 : t * 128 + 128] = cells[t]
                else:
                    big[PR, l, :, r : r + 16, :] = new_p * mask[:, r : r + 16, :]
                    big[TH, l, :, r : r + 16, :] = new_t
            return 0

        lax.fori_loop(0, NL, body, 0, unroll=UNROLL)

    for d in far:
        scatter(d).wait_recv()
    total = half[pl.ds(pl.multiple_of(me * CHUNK, 8), CHUNK), :]
    for d in range(1, 16):
        total = total + xy_recv[d]
    red[...] = total

    def across(d):
        return remote(red, z_recv.at[d], z_send.at[d], z_got.at[d], column_dev(d))

    for d in deep:
        across(d).start()

    for copy in x_copies:
        copy.wait()
    near = lanes((32, 128)) < 64

    def unpack_x(f, _):
        for i in range(16):
            shift_a, shift_b = (128 - 8 * i) % 128, (128 - 8 * (i + 1)) % 128
            a, b = xr[0, f], xr[1, f]
            a = pltpu.roll(a, shift_a, 1) if shift_a else a
            b = pltpu.roll(b, shift_b, 1) if shift_b else b
            r = TOP + 32 * (i % 2)
            big[f, i // 2, 3, r : r + 32, :] = jnp.where(near, a, b)
        return 0

    lax.fori_loop(0, 6, unpack_x, 0)

    slot8 = lanes((8, 128)) // 16

    def pack_c(f, _):
        for s, r in ((0, TOP), (1, BOT - 8)):
            acc = None
            for l in range(NL):
                shift = (8 + 16 * l) % 128
                cells = pltpu.roll(big[f, l, 3, r : r + 8, :], shift, 1)
                acc = cells if acc is None else jnp.where(slot8 == l, cells, acc)
            cs[s, f] = acc
        return 0

    lax.fori_loop(0, 6, pack_c, 0)
    c_copies = [remote(cs.at[s], cr.at[s], ch_send.at[s], ch_got.at[s], rows_to[s]) for s in range(2)]
    for copy in c_copies:
        copy.start()

    def mask_p(l, _):
        big[PR, l, 3, TOP:BOT, :] = big[PR, l, 3, TOP:BOT, :] * mask[3, TOP:BOT, :]
        return 0

    lax.fori_loop(0, NL, mask_p, 0)
    winds((24, 40, 56))
    for d in deep:
        across(d).wait_recv()
    total = red[...]
    for d in range(1, 8):
        total = total + z_recv[d]

    def chunk_of(q):
        return modes.at[pl.ds(pl.multiple_of(core * HALF + q * CHUNK, 8), CHUNK), :]

    modes[pl.ds(pl.multiple_of(core * HALF + me * CHUNK, 8), CHUNK), :] = total

    def gather(d):
        return remote(chunk_of(me), chunk_of(me), ag_send.at[d], ag_got.at[d], plane_dev(d))

    def forward(d):
        x, y = (px + 4 - d % 4) % 4, (py + 4 - d // 4) % 4
        ref = chunk_of(y * 4 + x)
        return remote(ref, ref, fw_send.at[d], fw_got.at[d], partner)

    for d in far:
        gather(d).start()
    forward(0).start()

    for copy in y_copies:
        copy.wait()
    for copy in c_copies:
        copy.wait()

    def put(f, l, r, cells):
        big[f, l, 0:3, r : r + 8, :] = cells

    def other(cells):
        return pltpu.roll(cells, 4, 1)

    def unpack_y(l, _):
        for s, r in ((0, BOT), (1, TOP - 8)):
            near_four = low_rows if s == 0 else sub >= 4
            one, two = yr[s, l, 0], yr[s, l, 1]
            put(U, l, r, one if s == 0 else other(one))
            p = two if s == 0 else other(two)
            put(PR, l, r, jnp.where(near_four, p, 0.0) * mask[0:3, r : r + 8, :])
            put(SS, l, r, other(two) if s == 0 else two)
        return 0

    def unpack_first(l, _):
        for s, r in ((0, BOT), (1, TOP - 8)):
            one, three = yr[s, l, 0], yr[s, l, 2]
            w_1 = other(one) if s == 0 else one
            t_1 = pltpu.roll(three, 3 if s == 0 else 6, 1)
            theta = jnp.where((sub < 2) if s == 0 else (sub >= 6), t_1 + 0.5 * w_1, 0.0)
            put(TH, l, r, theta)
            put(W, l, r, w_1 + 0.25 * edge_z(l, r) - 0.5 * theta)
            along = edge(PR, l, r + 1) - edge(PR, l, r - 1)
            put(V, l, r, jnp.where(sub == (0 if s == 0 else 7), three, three + 0.25 * along))
        return 0

    lax.fori_loop(0, NL, unpack_y, 0)
    lax.fori_loop(0, NL, unpack_first, 0)

    def unpack_c(f, _):
        for s, r in ((0, BOT), (1, TOP - 8)):
            for l in range(NL):
                big[f, l, 3, r : r + 8, :] = pltpu.roll(cr[s, f], (128 - 8 - 16 * l) % 128, 1)
        return 0

    lax.fori_loop(0, 6, unpack_c, 0)

    def mask_c(l, _):
        for r in (TOP - 8, BOT):
            big[PR, l, 3, r : r + 8, :] = big[PR, l, 3, r : r + 8, :] * mask[3, r : r + 8, :]
        return 0

    lax.fori_loop(0, NL, mask_c, 0)

    every = range(8, 88, 16)
    winds((8, 72))
    pressure(every)
    winds(every)
    pressure(every)
    winds(every)
    for d in far:
        gather(d).wait_recv()
        forward(d).start()
    pressure(range(TOP, BOT, 16), last=True)

    for d in range(16):
        forward(d).wait()
    for d in far:
        scatter(d).wait_send()
        gather(d).wait_send()
    for d in deep:
        across(d).wait_send()


def sum_modes(state, driving, sound, tab_x, tab_y):
    vmem = pl.BlockSpec(memory_space=pltpu.VMEM)
    hbm = pl.BlockSpec(memory_space=pltpu.HBM)
    dma = pltpu.SemaphoreType.DMA
    return pl.pallas_call(
        mode_kernel,
        out_shape=(
            jax.ShapeDtypeStruct((2 * HALF, 128), F32),
            jax.ShapeDtypeStruct((NF, NL, ROWS, COLS), F32),
            jax.ShapeDtypeStruct((384, COLS), BF16),
            jax.ShapeDtypeStruct((64, 256), BF16),
        ),
        in_specs=[hbm] * 5,
        out_specs=(vmem, vmem, vmem, vmem),
        scratch_shapes=[
            pltpu.VMEM((6, NL, 4, 96, 128), F32),
            pltpu.VMEM((NF, NL, ROWS, COLS), F32),
            pltpu.VMEM((MODES, COLS), F32),
            pltpu.VMEM((64, 128), F32),
            pltpu.VMEM((256, COLS), BF16),
            pltpu.VMEM((64, 256), BF16),
            pltpu.VMEM((4, 96, 128), F32),
            pltpu.VMEM((2 * HALF, 128), F32),
            pltpu.VMEM((HALF, 128), F32),
            pltpu.VMEM((HALF, 128), F32),
            pltpu.VMEM((16, CHUNK, 128), F32),
            pltpu.VMEM((CHUNK, 128), F32),
            pltpu.VMEM((8, CHUNK, 128), F32),
            pltpu.VMEM((2, 6, 32, 128), F32),
            pltpu.VMEM((2, 6, 32, 128), F32),
            pltpu.VMEM((2, NL, 3, 3, 8, 128), F32),
            pltpu.VMEM((2, NL, 3, 3, 8, 128), F32),
            pltpu.VMEM((2, 6, 8, 128), F32),
            pltpu.VMEM((2, 6, 8, 128), F32),
            dma((NF, 3)), dma((NF,)), dma((3,)), dma((2,)), dma((2,)),
            dma((16,)), dma((16,)), dma((8,)), dma((8,)),
            dma((16,)), dma((16,)), dma((16,)), dma((16,)),
            dma((2,)), dma((2,)), dma((2,)), dma((2,)), dma((2,)), dma((2,)),
        ],
        compiler_params=pltpu.CompilerParams(
            collective_id=0, has_side_effects=True, vmem_limit_bytes=40 * 1024 * 1024
        ),
        name="sum_modes",
    )(*(pltpu.with_memory_space_constraint(a, pltpu.HBM) for a in (state, driving, sound, tab_x, tab_y)))


def back_kernel(rate, modes, xt3, yt3, adv, out, held, done, sem):
    side = lanes((64, 128)) < 64
    for f in range(NF):
        scaled = [
            modes[4 * f + q] * jnp.where(side, rate[f, 2 * q], rate[f, 2 * q + 1]) for q in range(4)
        ]
        high, low = split(jnp.concatenate(scaled, axis=1))
        held[f] = dot(yt3[...], jnp.concatenate([high, high, low, low], axis=0))

    def write(f):
        return pltpu.make_async_copy(done.at[f], out.at[f], sem.at[f])

    for f in range(NF):
        rows = []
        for q in range(4):
            both = held[f, :, 128 * q : 128 * q + 128]
            rows += [jnp.where(side, both, 0.0), jnp.where(side, 0.0, both)]
        high, low = split(jnp.concatenate(rows, axis=0))
        tendency = dot(jnp.concatenate([high, low, high], axis=1), xt3[...])
        done[f] = adv[f] - tendency.reshape(NL, ROWS, COLS)
        write(f).start()
    for f in range(NF):
        write(f).wait()


def nudge(rate, modes, xt3, yt3, adv):
    vmem = pl.BlockSpec(memory_space=pltpu.VMEM)
    return pl.pallas_call(
        back_kernel,
        out_shape=jax.ShapeDtypeStruct((NF, NL, ROWS, COLS), F32),
        in_specs=[pl.BlockSpec(memory_space=pltpu.SMEM)] + [vmem] * 4,
        out_specs=pl.BlockSpec(memory_space=pltpu.HBM),
        scratch_shapes=[
            pltpu.VMEM((NF, 64, 512), F32),
            pltpu.VMEM((NF, NL, ROWS, COLS), F32),
            pltpu.SemaphoreType.DMA((NF,)),
        ],
        compiler_params=pltpu.CompilerParams(vmem_limit_bytes=32 * 1024 * 1024),
        name="nudge",
    )(rate, modes, xt3, yt3, adv)


def solution(mesh):
    tab_x, tab_y = tables()

    def on_device(state, driving, rate, sound_square):
        modes, adv, xt3, yt3 = sum_modes(state, driving, sound_square, jnp.asarray(tab_x), jnp.asarray(tab_y))
        return nudge(rate, modes.reshape(20, 64, 128), xt3, yt3, adv)

    return jax.shard_map(
        on_device,
        mesh=mesh,
        in_specs=(P(None, None, "gy", "gx"), P(None, None, "gy", "gx"), P(), P(None, "gy", "gx")),
        out_specs=P(None, None, "gy", "gx"),
        check_vma=False,
    )
```

```python
import jax
import jax.numpy as jnp
import numpy as np
from jax import lax
from jax.experimental import pallas as pl
from jax.experimental.pallas import tpu as pltpu
from jax.sharding import PartitionSpec as P

MODES = 64
SUBSTEPS = 3
NX = 3072
NY = 2048
NF, NL, ROWS, COLS = 5, 8, 64, 384
GX, GY = 8, 32
F32, BF16 = jnp.float32, jnp.bfloat16
MESH = pl.DeviceIdType.MESH
TOP, BOT = 16, 80
HALF, CHUNK = 640, 40
UNROLL = 2
U, V, W, PR, TH, SS = range(6)


def basis(size):
    index = np.arange(size, dtype=np.int64)
    order = np.arange(MODES, dtype=np.int64)
    freq = np.where(order < MODES // 2, order, order - MODES // 2 + 1)
    wrapped = (freq[:, None] * (2 * index[None, :] + 1)) % (2 * size)
    phase = np.float32(np.pi) * wrapped.astype(np.float32) / np.float32(size)
    phase = phase.astype(np.float64)
    table = np.where(order[:, None] < MODES // 2, np.cos(phase), np.sin(phase))
    scaling = np.where(order == 0, 1.0 / size, 2.0 / size).astype(np.float32)
    table = table.astype(np.float32)
    return table, table * scaling[:, None]


def tables():
    basis_x, _ = basis(NX)
    basis_y, weight_y = basis(NY)
    tab_x = basis_x.reshape(MODES, GX, COLS).transpose(1, 0, 2)
    by_tile = basis_y.reshape(MODES, GY, ROWS).transpose(1, 2, 0)
    wy_tile = weight_y.reshape(MODES, GY, ROWS).transpose(1, 0, 2)
    return np.ascontiguousarray(tab_x), np.concatenate([wy_tile, by_tile], axis=2)


def lanes(shape):
    return lax.broadcasted_iota(jnp.int32, shape, len(shape) - 1)


def split(x):
    high = x.astype(BF16)
    return high, (x - high.astype(F32)).astype(BF16)


def y_table(pair):
    lane = lanes(pair.shape)
    high = pair.astype(BF16).astype(F32)
    first = jnp.where(lane < 64, high, pair - high)
    second = jnp.where(lane < 64, high, 0.0)
    return jnp.concatenate([first, second], axis=1).astype(BF16)


def dot(a, b):
    return jnp.dot(a, b, preferred_element_type=F32)


def mode_kernel(
    state, driving, sound, tab_x, tab_y,
    modes, adv, xt3, yt3,
    big, drv, tx, ty, wx, wy, mask, local, half, core_recv, xy_recv, red, z_recv,
    xs, xr, ys, yr, cs, cr,
    ld_sem, drv_sem, snd_sem, tab_sem, core_sem, xy_send, xy_got, z_send, z_got,
    ag_send, ag_got, fw_send, fw_got, xh_send, xh_got, yh_send, yh_got, ch_send, ch_got,
):
    gx, gy = lax.axis_index("gx"), lax.axis_index("gy")
    py, zlo = gx // 2, gx % 2
    core, px, zhi = gy % 2, (gy // 2) % 4, gy // 8
    pz = zhi * 2 + zlo
    me = py * 4 + px

    def at(x, y, z, c):
        return {"gx": y * 2 + z % 2, "gy": ((z // 2) * 4 + x) * 2 + c}

    partner = at(px, py, pz, 1 - core)

    def plane(d):
        return (px + d % 4) % 4, (py + d // 4) % 4

    def plane_dev(d):
        x, y = plane(d)
        return at(x, y, pz, core)

    def column_dev(d):
        return at(px, py, (pz + d) % 8, core)

    left, right = {"gx": (gx + GX - 1) % GX, "gy": gy}, {"gx": (gx + 1) % GX, "gy": gy}
    above, below = {"gx": gx, "gy": (gy + GY - 1) % GY}, {"gx": gx, "gy": (gy + 1) % GY}
    sides = (left, right)
    rows_to = (above, below)

    far = sorted(range(1, 16), key=lambda d: -(min(d % 4, 4 - d % 4) + min(d // 4, 4 - d // 4)))
    deep = sorted(range(1, 8), key=lambda d: -min(d, 8 - d))

    inner = {"x": (gx > 0, gx < GX - 1), "y": (gy > 0, gy < GY - 1), "c": (gy > 0, gy < GY - 1)}

    @pl.when(gx == GX - 1)
    def _():
        xr[0] = jnp.zeros_like(xr[0])

    @pl.when(gx == 0)
    def _():
        xr[1] = jnp.zeros_like(xr[1])

    @pl.when(gy == GY - 1)
    def _():
        yr[0] = jnp.zeros_like(yr[0])
        cr[0] = jnp.zeros_like(cr[0])

    @pl.when(gy == 0)
    def _():
        yr[1] = jnp.zeros_like(yr[1])
        cr[1] = jnp.zeros_like(cr[1])

    def start_bands(name, copies):
        for s in range(2):
            pl.when(inner[name][s])(copies[s].start)

    def wait_bands(name, copies):
        for s in range(2):
            pl.when(inner[name][s])(copies[s].wait_send)
            pl.when(inner[name][1 - s])(copies[s].wait_recv)

    barrier = pltpu.get_barrier_semaphore()
    peers = [partner] + [plane_dev(d) for d in far] + [column_dev(d) for d in deep]
    peers += [left, right, above, below]
    for peer in peers:
        pl.semaphore_signal(barrier, inc=1, device_id=peer, device_id_type=MESH)

    def remote(src, dst, send, recv, dev):
        return pltpu.make_async_remote_copy(
            src_ref=src, dst_ref=dst, send_sem=send, recv_sem=recv, device_id=dev, device_id_type=MESH
        )

    def load(f, t):
        return pltpu.make_async_copy(
            state.at[f, :, :, pl.ds(t * 128, 128)], big.at[f, :, t, pl.ds(TOP, ROWS), :], ld_sem.at[f, t]
        )

    def load_drv(f):
        return pltpu.make_async_copy(driving.at[f], drv.at[f], drv_sem.at[f])

    def load_sound(t):
        return pltpu.make_async_copy(
            sound.at[:, :, pl.ds(t * 128, 128)], big.at[SS, :, t, pl.ds(TOP, ROWS), :], snd_sem.at[t]
        )

    get_tx = pltpu.make_async_copy(tab_x.at[gx], tx, tab_sem.at[0])
    get_ty = pltpu.make_async_copy(tab_y.at[gy], ty, tab_sem.at[1])
    get_tx.start()
    get_ty.start()
    def nth(i):
        return jnp.where(core == 0, NF - 1 - i, i)

    for i in range(NF):
        for t in range(3):
            load(nth(i), t).start()
        load_drv(nth(i)).start()
    for t in range(3):
        load_sound(t).start()

    get_tx.wait()
    get_ty.wait()
    b_x = tx[...]
    k_row = lax.broadcasted_iota(jnp.int32, b_x.shape, 0)
    w_x = b_x * jnp.where(k_row == 0, np.float32(1.0 / NX), np.float32(2.0 / NX))
    w_hi, w_lo = split(w_x)
    wx[...] = jnp.concatenate([w_hi, w_hi, w_lo, w_lo], axis=0)
    b_hi, b_lo = split(b_x)
    xt3[...] = jnp.concatenate([b_hi, b_hi, b_hi, b_hi, b_lo, b_lo], axis=0)
    pair = ty[...]
    lane2 = lanes(pair.shape)
    turned = pltpu.roll(pair, 64, 1)
    wy[...] = y_table(jnp.where(lane2 < 64, pair, turned))
    yt3[...] = y_table(jnp.where(lane2 < 64, turned, pair))

    row = lax.broadcasted_iota(jnp.int32, (96, 128), 0)
    lane = lanes((96, 128))
    row_ok = ((row >= TOP) | (gy > 0)) & ((row < BOT) | (gy < GY - 1))
    col_ok = jnp.where(lane < 64, jnp.where(gx < GX - 1, 1.0, 0.0), jnp.where(gx > 0, 1.0, 0.0))
    row_ok = jnp.where(row_ok, 1.0, 0.0)
    for t in range(3):
        mask[t] = row_ok
    mask[3] = row_ok * col_ok

    def project(i, _):
        f = nth(i)
        for t in range(3):
            load(f, t).wait()
        load_drv(f).wait()
        diff = jnp.concatenate(
            [
                big[f, :, t, TOP:BOT, :].reshape(512, 128)
                - drv[f, :, :, t * 128 : (t + 1) * 128].reshape(512, 128)
                for t in range(3)
            ],
            axis=1,
        )
        high, low = split(diff)
        nt = (((1,), (1,)), ((), ()))
        a = lax.dot_general(high, wx[...], nt, preferred_element_type=F32)
        b = lax.dot_general(low, wx[0:128], nt, preferred_element_type=F32)
        part = a[:, :128] + (a[:, 128:] + b)
        side = lanes((64, 128))
        pairs = [
            jnp.where(side < 64, part[128 * q : 128 * q + 64], part[128 * q + 64 : 128 * q + 128])
            for q in range(4)
        ]
        high, low = split(jnp.concatenate(pairs, axis=1))
        rhs = jnp.concatenate([high, high, low, low], axis=0)
        out = dot(wy[...], rhs)
        for q in range(4):
            local[pl.ds(pl.multiple_of((f * 4 + q) * 64, 64), 64), :] = out[:, 128 * q : 128 * q + 128]
        return 0

    lax.fori_loop(0, 3, project, 0)
    pl.semaphore_wait(barrier, len(peers))

    give = remote(
        local.at[pl.ds(pl.multiple_of((1 - core) * HALF, 8), HALF), :], core_recv, core_sem.at[0], core_sem.at[1], partner
    )
    give.start()
    lax.fori_loop(3, NF, project, 0)

    for t in range(3):
        load_sound(t).wait()
    slot = lanes((32, 128)) // 8

    def pack_x(f, _):
        for side, tile in ((0, 0), (1, 2)):
            acc = None
            for i in range(16):
                cells = big[f, i // 2, tile, TOP + 32 * (i % 2) : TOP + 32 * (i % 2) + 32, :]
                shift = (8 * (i + side)) % 128
                cells = pltpu.roll(cells, shift, 1) if shift else cells
                acc = cells if acc is None else jnp.where(slot == i, cells, acc)
            xs[side, f] = acc
        return 0

    lax.fori_loop(0, 6, pack_x, 0)
    sub = lax.broadcasted_iota(jnp.int32, (3, 8, 128), 1)
    low_rows = sub < 4

    def edge(f, l, r):
        return big[f, l, 0:3, r : r + 8, :]

    def edge_z(l, r):
        up = edge(PR, jnp.minimum(l + 1, NL - 1), r) * jnp.where(l < NL - 1, 1.0, 0.0)
        down = edge(PR, jnp.maximum(l - 1, 0), r) * jnp.where(l > 0, 1.0, 0.0)
        return up - down

    def pack_y(l, _):
        for s, r in ((0, TOP), (1, BOT - 8)):
            def joined(a, b):
                if s == 0:
                    return jnp.where(low_rows, a, pltpu.roll(b, 4, 1))
                return jnp.where(low_rows, pltpu.roll(a, 4, 1), b)

            w_1 = edge(W, l, r) - 0.25 * edge_z(l, r) + 0.5 * edge(TH, l, r)
            t_1 = edge(TH, l, r) - 0.5 * w_1
            v_0 = edge(V, l, r)
            v_1 = v_0 - 0.25 * (edge(PR, l, r + 1) - edge(PR, l, r - 1))
            first = sub == (0 if s == 0 else 7)
            v = jnp.where(first, v_0, v_1)
            ys[s, l, 0] = joined(edge(U, l, r), w_1)
            ys[s, l, 1] = joined(edge(PR, l, r), edge(SS, l, r))
            if s == 0:
                ys[s, l, 2] = jnp.where(sub < 5, v, pltpu.roll(t_1, 5, 1))
            else:
                ys[s, l, 2] = jnp.where(sub >= 3, v, pltpu.roll(t_1, 2, 1))
        return 0

    lax.fori_loop(0, NL, pack_y, 0)
    give.wait()
    half[...] = local[pl.ds(pl.multiple_of(core * HALF, 8), HALF), :] + core_recv[...]

    y_copies = [remote(ys.at[s], yr.at[s], yh_send.at[s], yh_got.at[s], rows_to[s]) for s in range(2)]
    start_bands("y", y_copies)

    def scatter(d):
        x, y = plane(d)
        return remote(
            half.at[pl.ds(pl.multiple_of((y * 4 + x) * CHUNK, 8), CHUNK), :],
            xy_recv.at[d], xy_send.at[d], xy_got.at[d], plane_dev(d),
        )

    for d in far:
        scatter(d).start()

    x_copies = [remote(xs.at[s], xr.at[s], xh_send.at[s], xh_got.at[s], sides[s]) for s in range(2)]
    start_bands("x", x_copies)

    lane4 = lanes((4, 16, 128))
    at_end, at_start = lane4 == 127, lane4 == 0

    def across_x(c):
        fwd, back = pltpu.roll(c, 127, 2), pltpu.roll(c, 1, 2)
        fwd = jnp.where(at_end, jnp.concatenate([fwd[1:], fwd[:1]], axis=0), fwd)
        back = jnp.where(at_start, jnp.concatenate([back[3:], back[:3]], axis=0), back)
        return fwd - back

    def get(f, l, r):
        return big[f, l, :, r : r + 16, :]

    def vertical(f, l, r):
        up = get(f, jnp.minimum(l + 1, NL - 1), r) * jnp.where(l < NL - 1, 1.0, 0.0)
        down = get(f, jnp.maximum(l - 1, 0), r) * jnp.where(l > 0, 1.0, 0.0)
        return up - down

    def winds(rows):
        def body(l, _):
            for r in rows:
                ok = mask[:, r : r + 16, :]
                big[U, l, :, r : r + 16, :] = (get(U, l, r) - 0.25 * across_x(get(PR, l, r))) * ok
                along = get(PR, l, r + 1) - get(PR, l, r - 1)
                big[V, l, :, r : r + 16, :] = (get(V, l, r) - 0.25 * along) * ok
                big[W, l, :, r : r + 16, :] = get(W, l, r) - 0.25 * vertical(PR, l, r) + 0.5 * get(TH, l, r)
            return 0

        lax.fori_loop(0, NL, body, 0, unroll=UNROLL)

    def pressure(rows, last=False):
        def body(l, _):
            for r in rows:
                along = get(V, l, r + 1) - get(V, l, r - 1)
                diverge = across_x(get(U, l, r)) + along + vertical(W, l, r)
                new_p = get(PR, l, r) - 0.25 * get(SS, l, r) * diverge
                new_t = get(TH, l, r) - 0.5 * get(W, l, r)
                if last:
                    done = (get(U, l, r), get(V, l, r), get(W, l, r), new_p, new_t)
                    for f, cells in enumerate(done):
                        for t in range(3):
                            adv[f, l, r - TOP : r - TOP + 16, t * 128 : t * 128 + 128] = cells[t]
                else:
                    big[PR, l, :, r : r + 16, :] = new_p * mask[:, r : r + 16, :]
                    big[TH, l, :, r : r + 16, :] = new_t
            return 0

        lax.fori_loop(0, NL, body, 0, unroll=UNROLL)

    for d in far:
        scatter(d).wait_recv()
    total = half[pl.ds(pl.multiple_of(me * CHUNK, 8), CHUNK), :]
    for d in range(1, 16):
        total = total + xy_recv[d]
    red[...] = total

    def across(d):
        return remote(red, z_recv.at[d], z_send.at[d], z_got.at[d], column_dev(d))

    for d in deep:
        across(d).start()

    wait_bands("x", x_copies)
    near = lanes((32, 128)) < 64

    def unpack_x(f, _):
        for i in range(16):
            shift_a, shift_b = (128 - 8 * i) % 128, (128 - 8 * (i + 1)) % 128
            a, b = xr[0, f], xr[1, f]
            a = pltpu.roll(a, shift_a, 1) if shift_a else a
            b = pltpu.roll(b, shift_b, 1) if shift_b else b
            r = TOP + 32 * (i % 2)
            big[f, i // 2, 3, r : r + 32, :] = jnp.where(near, a, b)
        return 0

    lax.fori_loop(0, 6, unpack_x, 0)

    slot8 = lanes((8, 128)) // 16

    def pack_c(f, _):
        for s, r in ((0, TOP), (1, BOT - 8)):
            acc = None
            for l in range(NL):
                shift = (8 + 16 * l) % 128
                cells = pltpu.roll(big[f, l, 3, r : r + 8, :], shift, 1)
                acc = cells if acc is None else jnp.where(slot8 == l, cells, acc)
            cs[s, f] = acc
        return 0

    lax.fori_loop(0, 6, pack_c, 0)
    c_copies = [remote(cs.at[s], cr.at[s], ch_send.at[s], ch_got.at[s], rows_to[s]) for s in range(2)]
    start_bands("c", c_copies)

    def mask_p(l, _):
        big[PR, l, 3, TOP:BOT, :] = big[PR, l, 3, TOP:BOT, :] * mask[3, TOP:BOT, :]
        return 0

    lax.fori_loop(0, NL, mask_p, 0)
    winds((24, 40, 56))
    for d in deep:
        across(d).wait_recv()
    total = red[...]
    for d in range(1, 8):
        total = total + z_recv[d]

    def chunk_of(q):
        return modes.at[pl.ds(pl.multiple_of(core * HALF + q * CHUNK, 8), CHUNK), :]

    modes[pl.ds(pl.multiple_of(core * HALF + me * CHUNK, 8), CHUNK), :] = total

    def gather(d):
        return remote(chunk_of(me), chunk_of(me), ag_send.at[d], ag_got.at[d], plane_dev(d))

    def forward(d):
        x, y = (px + 4 - d % 4) % 4, (py + 4 - d // 4) % 4
        ref = chunk_of(y * 4 + x)
        return remote(ref, ref, fw_send.at[d], fw_got.at[d], partner)

    for d in far:
        gather(d).start()
    forward(0).start()

    wait_bands("y", y_copies)
    wait_bands("c", c_copies)

    def put(f, l, r, cells):
        big[f, l, 0:3, r : r + 8, :] = cells

    def other(cells):
        return pltpu.roll(cells, 4, 1)

    def unpack_y(l, _):
        for s, r in ((0, BOT), (1, TOP - 8)):
            near_four = low_rows if s == 0 else sub >= 4
            one, two = yr[s, l, 0], yr[s, l, 1]
            put(U, l, r, one if s == 0 else other(one))
            p = two if s == 0 else other(two)
            put(PR, l, r, jnp.where(near_four, p, 0.0) * mask[0:3, r : r + 8, :])
            put(SS, l, r, other(two) if s == 0 else two)
        return 0

    def unpack_first(l, _):
        for s, r in ((0, BOT), (1, TOP - 8)):
            one, three = yr[s, l, 0], yr[s, l, 2]
            w_1 = other(one) if s == 0 else one
            t_1 = pltpu.roll(three, 3 if s == 0 else 6, 1)
            theta = jnp.where((sub < 2) if s == 0 else (sub >= 6), t_1 + 0.5 * w_1, 0.0)
            put(TH, l, r, theta)
            put(W, l, r, w_1 + 0.25 * edge_z(l, r) - 0.5 * theta)
            along = edge(PR, l, r + 1) - edge(PR, l, r - 1)
            put(V, l, r, jnp.where(sub == (0 if s == 0 else 7), three, three + 0.25 * along))
        return 0

    lax.fori_loop(0, NL, unpack_y, 0)
    lax.fori_loop(0, NL, unpack_first, 0)

    def unpack_c(f, _):
        for s, r in ((0, BOT), (1, TOP - 8)):
            for l in range(NL):
                big[f, l, 3, r : r + 8, :] = pltpu.roll(cr[s, f], (128 - 8 - 16 * l) % 128, 1)
        return 0

    lax.fori_loop(0, 6, unpack_c, 0)

    def mask_c(l, _):
        for r in (TOP - 8, BOT):
            big[PR, l, 3, r : r + 8, :] = big[PR, l, 3, r : r + 8, :] * mask[3, r : r + 8, :]
        return 0

    lax.fori_loop(0, NL, mask_c, 0)

    every = range(8, 88, 16)
    winds((8, 72))
    pressure(every)
    winds(every)
    pressure(every)
    winds(every)
    for d in far:
        gather(d).wait_recv()
        forward(d).start()
    pressure(range(TOP, BOT, 16), last=True)

    for d in range(16):
        forward(d).wait()
    for d in far:
        scatter(d).wait_send()
        gather(d).wait_send()
    for d in deep:
        across(d).wait_send()


def sum_modes(state, driving, sound, tab_x, tab_y):
    vmem = pl.BlockSpec(memory_space=pltpu.VMEM)
    hbm = pl.BlockSpec(memory_space=pltpu.HBM)
    dma = pltpu.SemaphoreType.DMA
    return pl.pallas_call(
        mode_kernel,
        out_shape=(
            jax.ShapeDtypeStruct((2 * HALF, 128), F32),
            jax.ShapeDtypeStruct((NF, NL, ROWS, COLS), F32),
            jax.ShapeDtypeStruct((384, COLS), BF16),
            jax.ShapeDtypeStruct((64, 256), BF16),
        ),
        in_specs=[hbm] * 5,
        out_specs=(vmem, vmem, vmem, vmem),
        scratch_shapes=[
            pltpu.VMEM((6, NL, 4, 96, 128), F32),
            pltpu.VMEM((NF, NL, ROWS, COLS), F32),
            pltpu.VMEM((MODES, COLS), F32),
            pltpu.VMEM((64, 128), F32),
            pltpu.VMEM((256, COLS), BF16),
            pltpu.VMEM((64, 256), BF16),
            pltpu.VMEM((4, 96, 128), F32),
            pltpu.VMEM((2 * HALF, 128), F32),
            pltpu.VMEM((HALF, 128), F32),
            pltpu.VMEM((HALF, 128), F32),
            pltpu.VMEM((16, CHUNK, 128), F32),
            pltpu.VMEM((CHUNK, 128), F32),
            pltpu.VMEM((8, CHUNK, 128), F32),
            pltpu.VMEM((2, 6, 32, 128), F32),
            pltpu.VMEM((2, 6, 32, 128), F32),
            pltpu.VMEM((2, NL, 3, 3, 8, 128), F32),
            pltpu.VMEM((2, NL, 3, 3, 8, 128), F32),
            pltpu.VMEM((2, 6, 8, 128), F32),
            pltpu.VMEM((2, 6, 8, 128), F32),
            dma((NF, 3)), dma((NF,)), dma((3,)), dma((2,)), dma((2,)),
            dma((16,)), dma((16,)), dma((8,)), dma((8,)),
            dma((16,)), dma((16,)), dma((16,)), dma((16,)),
            dma((2,)), dma((2,)), dma((2,)), dma((2,)), dma((2,)), dma((2,)),
        ],
        compiler_params=pltpu.CompilerParams(
            collective_id=0, has_side_effects=True, vmem_limit_bytes=40 * 1024 * 1024
        ),
        name="sum_modes",
    )(*(pltpu.with_memory_space_constraint(a, pltpu.HBM) for a in (state, driving, sound, tab_x, tab_y)))


def back_kernel(rate, modes, xt3, yt3, adv, out, held, done, sem):
    side = lanes((64, 128)) < 64
    for f in range(NF):
        scaled = [
            modes[4 * f + q] * jnp.where(side, rate[f, 2 * q], rate[f, 2 * q + 1]) for q in range(4)
        ]
        high, low = split(jnp.concatenate(scaled, axis=1))
        held[f] = dot(yt3[...], jnp.concatenate([high, high, low, low], axis=0))

    def write(f):
        return pltpu.make_async_copy(done.at[f], out.at[f], sem.at[f])

    for f in range(NF):
        rows = []
        for q in range(4):
            both = held[f, :, 128 * q : 128 * q + 128]
            rows += [jnp.where(side, both, 0.0), jnp.where(side, 0.0, both)]
        high, low = split(jnp.concatenate(rows, axis=0))
        tendency = dot(jnp.concatenate([high, low, high], axis=1), xt3[...])
        done[f] = adv[f] - tendency.reshape(NL, ROWS, COLS)
        write(f).start()
    for f in range(NF):
        write(f).wait()


def nudge(rate, modes, xt3, yt3, adv):
    vmem = pl.BlockSpec(memory_space=pltpu.VMEM)
    return pl.pallas_call(
        back_kernel,
        out_shape=jax.ShapeDtypeStruct((NF, NL, ROWS, COLS), F32),
        in_specs=[pl.BlockSpec(memory_space=pltpu.SMEM)] + [vmem] * 4,
        out_specs=pl.BlockSpec(memory_space=pltpu.HBM),
        scratch_shapes=[
            pltpu.VMEM((NF, 64, 512), F32),
            pltpu.VMEM((NF, NL, ROWS, COLS), F32),
            pltpu.SemaphoreType.DMA((NF,)),
        ],
        compiler_params=pltpu.CompilerParams(vmem_limit_bytes=32 * 1024 * 1024),
        name="nudge",
    )(rate, modes, xt3, yt3, adv)


def solution(mesh):
    tab_x, tab_y = tables()

    def on_device(state, driving, rate, sound_square):
        modes, adv, xt3, yt3 = sum_modes(state, driving, sound_square, jnp.asarray(tab_x), jnp.asarray(tab_y))
        return nudge(rate, modes.reshape(20, 64, 128), xt3, yt3, adv)

    return jax.shard_map(
        on_device,
        mesh=mesh,
        in_specs=(P(None, None, "gy", "gx"), P(None, None, "gy", "gx"), P(), P(None, "gy", "gx")),
        out_specs=P(None, None, "gy", "gx"),
        check_vma=False,
    )
```

```python
import jax
import jax.numpy as jnp
import numpy as np
from jax import lax
from jax.experimental import pallas as pl
from jax.experimental.pallas import tpu as pltpu
from jax.sharding import PartitionSpec as P

MODES = 64
SUBSTEPS = 3
NX = 3072
NY = 2048
NF, NL, ROWS, COLS = 5, 8, 64, 384
GX, GY = 8, 32
F32, BF16 = jnp.float32, jnp.bfloat16
MESH = pl.DeviceIdType.MESH
TOP, BOT = 16, 80
HALF, CHUNK = 640, 40
UNROLL = 2
U, V, W, PR, TH, SS = range(6)


def basis(size):
    index = np.arange(size, dtype=np.int64)
    order = np.arange(MODES, dtype=np.int64)
    freq = np.where(order < MODES // 2, order, order - MODES // 2 + 1)
    wrapped = (freq[:, None] * (2 * index[None, :] + 1)) % (2 * size)
    phase = np.float32(np.pi) * wrapped.astype(np.float32) / np.float32(size)
    phase = phase.astype(np.float64)
    table = np.where(order[:, None] < MODES // 2, np.cos(phase), np.sin(phase))
    scaling = np.where(order == 0, 1.0 / size, 2.0 / size).astype(np.float32)
    table = table.astype(np.float32)
    return table, table * scaling[:, None]


def tables():
    basis_x, _ = basis(NX)
    basis_y, weight_y = basis(NY)
    tab_x = basis_x.reshape(MODES, GX, COLS).transpose(1, 0, 2)
    by_tile = basis_y.reshape(MODES, GY, ROWS).transpose(1, 2, 0)
    wy_tile = weight_y.reshape(MODES, GY, ROWS).transpose(1, 0, 2)
    return np.ascontiguousarray(tab_x), np.concatenate([wy_tile, by_tile], axis=2)


def lanes(shape):
    return lax.broadcasted_iota(jnp.int32, shape, len(shape) - 1)


def split(x):
    high = x.astype(BF16)
    return high, (x - high.astype(F32)).astype(BF16)


def y_table(pair):
    lane = lanes(pair.shape)
    high = pair.astype(BF16).astype(F32)
    first = jnp.where(lane < 64, high, pair - high)
    second = jnp.where(lane < 64, high, 0.0)
    return jnp.concatenate([first, second], axis=1).astype(BF16)


def dot(a, b):
    return jnp.dot(a, b, preferred_element_type=F32)


def mode_kernel(
    state, driving, sound, tab_x, tab_y,
    modes, adv, xt3, yt3,
    big, drv, tx, ty, wx, wy, mask, local, half, core_recv, xy_recv, red, z_recv,
    xs, xr, ys, yr, cs, cr,
    ld_sem, drv_sem, snd_sem, tab_sem, core_sem, xy_send, xy_got, z_send, z_got,
    ag_send, ag_got, fw_send, fw_got, xh_send, xh_got, yh_send, yh_got, ch_send, ch_got,
):
    gx, gy = lax.axis_index("gx"), lax.axis_index("gy")
    py, zlo = gx // 2, gx % 2
    core, px, zhi = gy % 2, (gy // 2) % 4, gy // 8
    pz = zhi * 2 + zlo
    me = py * 4 + px

    def at(x, y, z, c):
        return {"gx": y * 2 + z % 2, "gy": ((z // 2) * 4 + x) * 2 + c}

    partner = at(px, py, pz, 1 - core)

    def plane(d):
        return (px + d % 4) % 4, (py + d // 4) % 4

    def plane_dev(d):
        x, y = plane(d)
        return at(x, y, pz, core)

    def column_dev(d):
        return at(px, py, (pz + d) % 8, core)

    left, right = {"gx": (gx + GX - 1) % GX, "gy": gy}, {"gx": (gx + 1) % GX, "gy": gy}
    above, below = {"gx": gx, "gy": (gy + GY - 1) % GY}, {"gx": gx, "gy": (gy + 1) % GY}
    sides = (left, right)
    rows_to = (above, below)

    far = sorted(range(1, 16), key=lambda d: -(min(d % 4, 4 - d % 4) + min(d // 4, 4 - d // 4)))
    deep = sorted(range(1, 8), key=lambda d: -min(d, 8 - d))

    inner = {"x": (gx > 0, gx < GX - 1), "y": (gy > 0, gy < GY - 1), "c": (gy > 0, gy < GY - 1)}

    @pl.when(gx == GX - 1)
    def _():
        xr[0] = jnp.zeros_like(xr[0])

    @pl.when(gx == 0)
    def _():
        xr[1] = jnp.zeros_like(xr[1])

    @pl.when(gy == GY - 1)
    def _():
        yr[0] = jnp.zeros_like(yr[0])
        cr[0] = jnp.zeros_like(cr[0])

    @pl.when(gy == 0)
    def _():
        yr[1] = jnp.zeros_like(yr[1])
        cr[1] = jnp.zeros_like(cr[1])

    def start_bands(name, copies):
        for s in range(2):
            pl.when(inner[name][s])(copies[s].start)

    def wait_bands(name, copies):
        for s in range(2):
            pl.when(inner[name][s])(copies[s].wait_send)
            pl.when(inner[name][1 - s])(copies[s].wait_recv)

    barrier = pltpu.get_barrier_semaphore()
    peers = [partner] + [plane_dev(d) for d in far] + [column_dev(d) for d in deep]
    peers += [left, right, above, below]
    for peer in peers:
        pl.semaphore_signal(barrier, inc=1, device_id=peer, device_id_type=MESH)

    def remote(src, dst, send, recv, dev):
        return pltpu.make_async_remote_copy(
            src_ref=src, dst_ref=dst, send_sem=send, recv_sem=recv, device_id=dev, device_id_type=MESH
        )

    def load(f, t):
        return pltpu.make_async_copy(
            state.at[f, :, :, pl.ds(t * 128, 128)], big.at[f, :, t, pl.ds(TOP, ROWS), :], ld_sem.at[f, t]
        )

    def load_drv(f):
        return pltpu.make_async_copy(driving.at[f], drv.at[f], drv_sem.at[f])

    def load_sound(t):
        return pltpu.make_async_copy(
            sound.at[:, :, pl.ds(t * 128, 128)], big.at[SS, :, t, pl.ds(TOP, ROWS), :], snd_sem.at[t]
        )

    get_tx = pltpu.make_async_copy(tab_x.at[gx], tx, tab_sem.at[0])
    get_ty = pltpu.make_async_copy(tab_y.at[gy], ty, tab_sem.at[1])
    get_tx.start()
    get_ty.start()
    def nth(i):
        return jnp.where(core == 0, NF - 1 - i, i)

    for i in range(NF):
        for t in range(3):
            load(nth(i), t).start()
        load_drv(nth(i)).start()
    for t in range(3):
        load_sound(t).start()

    get_tx.wait()
    get_ty.wait()
    b_x = tx[...]
    k_row = lax.broadcasted_iota(jnp.int32, b_x.shape, 0)
    w_x = b_x * jnp.where(k_row == 0, np.float32(1.0 / NX), np.float32(2.0 / NX))
    w_hi, w_lo = split(w_x)
    wx[...] = jnp.concatenate([w_hi, w_hi, w_lo, w_lo], axis=0)
    b_hi, b_lo = split(b_x)
    xt3[...] = jnp.concatenate([b_hi, b_hi, b_hi, b_hi, b_lo, b_lo], axis=0)
    pair = ty[...]
    lane2 = lanes(pair.shape)
    turned = pltpu.roll(pair, 64, 1)
    wy[...] = y_table(jnp.where(lane2 < 64, pair, turned))
    yt3[...] = y_table(jnp.where(lane2 < 64, turned, pair))

    row = lax.broadcasted_iota(jnp.int32, (96, 128), 0)
    lane = lanes((96, 128))
    row_ok = ((row >= TOP) | (gy > 0)) & ((row < BOT) | (gy < GY - 1))
    col_ok = jnp.where(lane < 64, jnp.where(gx < GX - 1, 1.0, 0.0), jnp.where(gx > 0, 1.0, 0.0))
    row_ok = jnp.where(row_ok, 1.0, 0.0)
    for t in range(3):
        mask[t] = row_ok
    mask[3] = row_ok * col_ok

    def project(i, _):
        f = nth(i)
        for t in range(3):
            load(f, t).wait()
        load_drv(f).wait()
        diff = jnp.concatenate(
            [
                big[f, :, t, TOP:BOT, :].reshape(512, 128)
                - drv[f, :, :, t * 128 : (t + 1) * 128].reshape(512, 128)
                for t in range(3)
            ],
            axis=1,
        )
        high, low = split(diff)
        nt = (((1,), (1,)), ((), ()))
        a = lax.dot_general(high, wx[...], nt, preferred_element_type=F32)
        b = lax.dot_general(low, wx[0:128], nt, preferred_element_type=F32)
        part = a[:, :128] + (a[:, 128:] + b)
        side = lanes((64, 128))
        pairs = [
            jnp.where(side < 64, part[128 * q : 128 * q + 64], part[128 * q + 64 : 128 * q + 128])
            for q in range(4)
        ]
        high, low = split(jnp.concatenate(pairs, axis=1))
        rhs = jnp.concatenate([high, high, low, low], axis=0)
        out = dot(wy[...], rhs)
        for q in range(4):
            local[pl.ds(pl.multiple_of((f * 4 + q) * 64, 64), 64), :] = out[:, 128 * q : 128 * q + 128]
        return 0

    lax.fori_loop(0, 3, project, 0)
    pl.semaphore_wait(barrier, len(peers))

    give = remote(
        local.at[pl.ds(pl.multiple_of((1 - core) * HALF, 8), HALF), :], core_recv, core_sem.at[0], core_sem.at[1], partner
    )
    give.start()
    lax.fori_loop(3, NF, project, 0)

    for t in range(3):
        load_sound(t).wait()
    sub = lax.broadcasted_iota(jnp.int32, (3, 8, 128), 1)
    low_rows = sub < 4

    def edge(f, l, r):
        return big[f, l, 0:3, r : r + 8, :]

    def edge_z(l, r):
        up = edge(PR, jnp.minimum(l + 1, NL - 1), r) * jnp.where(l < NL - 1, 1.0, 0.0)
        down = edge(PR, jnp.maximum(l - 1, 0), r) * jnp.where(l > 0, 1.0, 0.0)
        return up - down

    def pack_y(l, _):
        for s, r in ((0, TOP), (1, BOT - 8)):
            def joined(a, b):
                if s == 0:
                    return jnp.where(low_rows, a, pltpu.roll(b, 4, 1))
                return jnp.where(low_rows, pltpu.roll(a, 4, 1), b)

            w_1 = edge(W, l, r) - 0.25 * edge_z(l, r) + 0.5 * edge(TH, l, r)
            t_1 = edge(TH, l, r) - 0.5 * w_1
            v_0 = edge(V, l, r)
            v_1 = v_0 - 0.25 * (edge(PR, l, r + 1) - edge(PR, l, r - 1))
            first = sub == (0 if s == 0 else 7)
            v = jnp.where(first, v_0, v_1)
            ys[s, l, 0] = joined(edge(U, l, r), w_1)
            ys[s, l, 1] = joined(edge(PR, l, r), edge(SS, l, r))
            if s == 0:
                ys[s, l, 2] = jnp.where(sub < 5, v, pltpu.roll(t_1, 5, 1))
            else:
                ys[s, l, 2] = jnp.where(sub >= 3, v, pltpu.roll(t_1, 2, 1))
        return 0

    lax.fori_loop(0, NL, pack_y, 0)
    y_copies = [remote(ys.at[s], yr.at[s], yh_send.at[s], yh_got.at[s], rows_to[s]) for s in range(2)]
    start_bands("y", y_copies)

    slot = lanes((32, 128)) // 8

    def pack_x(f, _):
        for side, tile in ((0, 0), (1, 2)):
            acc = None
            for i in range(16):
                cells = big[f, i // 2, tile, TOP + 32 * (i % 2) : TOP + 32 * (i % 2) + 32, :]
                shift = (8 * (i + side)) % 128
                cells = pltpu.roll(cells, shift, 1) if shift else cells
                acc = cells if acc is None else jnp.where(slot == i, cells, acc)
            xs[side, f] = acc
        return 0

    lax.fori_loop(0, 6, pack_x, 0)
    give.wait()
    half[...] = local[pl.ds(pl.multiple_of(core * HALF, 8), HALF), :] + core_recv[...]

    def scatter(d):
        x, y = plane(d)
        return remote(
            half.at[pl.ds(pl.multiple_of((y * 4 + x) * CHUNK, 8), CHUNK), :],
            xy_recv.at[d], xy_send.at[d], xy_got.at[d], plane_dev(d),
        )

    for d in far:
        scatter(d).start()

    x_copies = [remote(xs.at[s], xr.at[s], xh_send.at[s], xh_got.at[s], sides[s]) for s in range(2)]
    start_bands("x", x_copies)

    lane4 = lanes((4, 16, 128))
    at_end, at_start = lane4 == 127, lane4 == 0

    def across_x(c):
        fwd, back = pltpu.roll(c, 127, 2), pltpu.roll(c, 1, 2)
        fwd = jnp.where(at_end, jnp.concatenate([fwd[1:], fwd[:1]], axis=0), fwd)
        back = jnp.where(at_start, jnp.concatenate([back[3:], back[:3]], axis=0), back)
        return fwd - back

    def get(f, l, r):
        return big[f, l, :, r : r + 16, :]

    def vertical(f, l, r):
        up = get(f, jnp.minimum(l + 1, NL - 1), r) * jnp.where(l < NL - 1, 1.0, 0.0)
        down = get(f, jnp.maximum(l - 1, 0), r) * jnp.where(l > 0, 1.0, 0.0)
        return up - down

    def winds(rows):
        def body(l, _):
            for r in rows:
                ok = mask[:, r : r + 16, :]
                big[U, l, :, r : r + 16, :] = (get(U, l, r) - 0.25 * across_x(get(PR, l, r))) * ok
                along = get(PR, l, r + 1) - get(PR, l, r - 1)
                big[V, l, :, r : r + 16, :] = (get(V, l, r) - 0.25 * along) * ok
                big[W, l, :, r : r + 16, :] = get(W, l, r) - 0.25 * vertical(PR, l, r) + 0.5 * get(TH, l, r)
            return 0

        lax.fori_loop(0, NL, body, 0, unroll=UNROLL)

    def pressure(rows, last=False):
        def body(l, _):
            for r in rows:
                along = get(V, l, r + 1) - get(V, l, r - 1)
                diverge = across_x(get(U, l, r)) + along + vertical(W, l, r)
                new_p = get(PR, l, r) - 0.25 * get(SS, l, r) * diverge
                new_t = get(TH, l, r) - 0.5 * get(W, l, r)
                if last:
                    done = (get(U, l, r), get(V, l, r), get(W, l, r), new_p, new_t)
                    for f, cells in enumerate(done):
                        for t in range(3):
                            adv[f, l, r - TOP : r - TOP + 16, t * 128 : t * 128 + 128] = cells[t]
                else:
                    big[PR, l, :, r : r + 16, :] = new_p * mask[:, r : r + 16, :]
                    big[TH, l, :, r : r + 16, :] = new_t
            return 0

        lax.fori_loop(0, NL, body, 0, unroll=UNROLL)

    for d in far:
        scatter(d).wait_recv()
    total = half[pl.ds(pl.multiple_of(me * CHUNK, 8), CHUNK), :]
    for d in range(1, 16):
        total = total + xy_recv[d]
    red[...] = total

    def across(d):
        return remote(red, z_recv.at[d], z_send.at[d], z_got.at[d], column_dev(d))

    for d in deep:
        across(d).start()

    wait_bands("x", x_copies)
    near = lanes((32, 128)) < 64

    def unpack_x(f, _):
        for i in range(16):
            shift_a, shift_b = (128 - 8 * i) % 128, (128 - 8 * (i + 1)) % 128
            a, b = xr[0, f], xr[1, f]
            a = pltpu.roll(a, shift_a, 1) if shift_a else a
            b = pltpu.roll(b, shift_b, 1) if shift_b else b
            r = TOP + 32 * (i % 2)
            big[f, i // 2, 3, r : r + 32, :] = jnp.where(near, a, b)
        return 0

    lax.fori_loop(0, 6, unpack_x, 0)

    slot8 = lanes((8, 128)) // 16

    def pack_c(f, _):
        for s, r in ((0, TOP), (1, BOT - 8)):
            acc = None
            for l in range(NL):
                shift = (8 + 16 * l) % 128
                cells = pltpu.roll(big[f, l, 3, r : r + 8, :], shift, 1)
                acc = cells if acc is None else jnp.where(slot8 == l, cells, acc)
            cs[s, f] = acc
        return 0

    lax.fori_loop(0, 6, pack_c, 0)
    c_copies = [remote(cs.at[s], cr.at[s], ch_send.at[s], ch_got.at[s], rows_to[s]) for s in range(2)]
    start_bands("c", c_copies)

    def mask_p(l, _):
        big[PR, l, 3, TOP:BOT, :] = big[PR, l, 3, TOP:BOT, :] * mask[3, TOP:BOT, :]
        return 0

    lax.fori_loop(0, NL, mask_p, 0)
    winds((24, 40, 56))
    for d in deep:
        across(d).wait_recv()
    total = red[...]
    for d in range(1, 8):
        total = total + z_recv[d]

    def chunk_of(q):
        return modes.at[pl.ds(pl.multiple_of(core * HALF + q * CHUNK, 8), CHUNK), :]

    modes[pl.ds(pl.multiple_of(core * HALF + me * CHUNK, 8), CHUNK), :] = total

    def gather(d):
        return remote(chunk_of(me), chunk_of(me), ag_send.at[d], ag_got.at[d], plane_dev(d))

    def forward(d):
        x, y = (px + 4 - d % 4) % 4, (py + 4 - d // 4) % 4
        ref = chunk_of(y * 4 + x)
        return remote(ref, ref, fw_send.at[d], fw_got.at[d], partner)

    for d in far:
        gather(d).start()
    forward(0).start()

    wait_bands("y", y_copies)
    wait_bands("c", c_copies)

    def put(f, l, r, cells):
        big[f, l, 0:3, r : r + 8, :] = cells

    def other(cells):
        return pltpu.roll(cells, 4, 1)

    def unpack_y(l, _):
        for s, r in ((0, BOT), (1, TOP - 8)):
            near_four = low_rows if s == 0 else sub >= 4
            one, two = yr[s, l, 0], yr[s, l, 1]
            put(U, l, r, one if s == 0 else other(one))
            p = two if s == 0 else other(two)
            put(PR, l, r, jnp.where(near_four, p, 0.0) * mask[0:3, r : r + 8, :])
            put(SS, l, r, other(two) if s == 0 else two)
        return 0

    def unpack_first(l, _):
        for s, r in ((0, BOT), (1, TOP - 8)):
            one, three = yr[s, l, 0], yr[s, l, 2]
            w_1 = other(one) if s == 0 else one
            t_1 = pltpu.roll(three, 3 if s == 0 else 6, 1)
            theta = jnp.where((sub < 2) if s == 0 else (sub >= 6), t_1 + 0.5 * w_1, 0.0)
            put(TH, l, r, theta)
            put(W, l, r, w_1 + 0.25 * edge_z(l, r) - 0.5 * theta)
            along = edge(PR, l, r + 1) - edge(PR, l, r - 1)
            put(V, l, r, jnp.where(sub == (0 if s == 0 else 7), three, three + 0.25 * along))
        return 0

    lax.fori_loop(0, NL, unpack_y, 0)
    lax.fori_loop(0, NL, unpack_first, 0)

    def unpack_c(f, _):
        for s, r in ((0, BOT), (1, TOP - 8)):
            for l in range(NL):
                big[f, l, 3, r : r + 8, :] = pltpu.roll(cr[s, f], (128 - 8 - 16 * l) % 128, 1)
        return 0

    lax.fori_loop(0, 6, unpack_c, 0)

    def mask_c(l, _):
        for r in (TOP - 8, BOT):
            big[PR, l, 3, r : r + 8, :] = big[PR, l, 3, r : r + 8, :] * mask[3, r : r + 8, :]
        return 0

    lax.fori_loop(0, NL, mask_c, 0)

    every = range(8, 88, 16)
    winds((8, 72))
    pressure(every)
    winds(every)
    pressure(every)
    winds(every)
    for d in far:
        gather(d).wait_recv()
        forward(d).start()
    pressure(range(TOP, BOT, 16), last=True)

    for d in range(16):
        forward(d).wait()
    for d in far:
        scatter(d).wait_send()
        gather(d).wait_send()
    for d in deep:
        across(d).wait_send()


def sum_modes(state, driving, sound, tab_x, tab_y):
    vmem = pl.BlockSpec(memory_space=pltpu.VMEM)
    hbm = pl.BlockSpec(memory_space=pltpu.HBM)
    dma = pltpu.SemaphoreType.DMA
    return pl.pallas_call(
        mode_kernel,
        out_shape=(
            jax.ShapeDtypeStruct((2 * HALF, 128), F32),
            jax.ShapeDtypeStruct((NF, NL, ROWS, COLS), F32),
            jax.ShapeDtypeStruct((384, COLS), BF16),
            jax.ShapeDtypeStruct((64, 256), BF16),
        ),
        in_specs=[hbm] * 5,
        out_specs=(vmem, vmem, vmem, vmem),
        scratch_shapes=[
            pltpu.VMEM((6, NL, 4, 96, 128), F32),
            pltpu.VMEM((NF, NL, ROWS, COLS), F32),
            pltpu.VMEM((MODES, COLS), F32),
            pltpu.VMEM((64, 128), F32),
            pltpu.VMEM((256, COLS), BF16),
            pltpu.VMEM((64, 256), BF16),
            pltpu.VMEM((4, 96, 128), F32),
            pltpu.VMEM((2 * HALF, 128), F32),
            pltpu.VMEM((HALF, 128), F32),
            pltpu.VMEM((HALF, 128), F32),
            pltpu.VMEM((16, CHUNK, 128), F32),
            pltpu.VMEM((CHUNK, 128), F32),
            pltpu.VMEM((8, CHUNK, 128), F32),
            pltpu.VMEM((2, 6, 32, 128), F32),
            pltpu.VMEM((2, 6, 32, 128), F32),
            pltpu.VMEM((2, NL, 3, 3, 8, 128), F32),
            pltpu.VMEM((2, NL, 3, 3, 8, 128), F32),
            pltpu.VMEM((2, 6, 8, 128), F32),
            pltpu.VMEM((2, 6, 8, 128), F32),
            dma((NF, 3)), dma((NF,)), dma((3,)), dma((2,)), dma((2,)),
            dma((16,)), dma((16,)), dma((8,)), dma((8,)),
            dma((16,)), dma((16,)), dma((16,)), dma((16,)),
            dma((2,)), dma((2,)), dma((2,)), dma((2,)), dma((2,)), dma((2,)),
        ],
        compiler_params=pltpu.CompilerParams(
            collective_id=0, has_side_effects=True, vmem_limit_bytes=40 * 1024 * 1024
        ),
        name="sum_modes",
    )(*(pltpu.with_memory_space_constraint(a, pltpu.HBM) for a in (state, driving, sound, tab_x, tab_y)))


def back_kernel(rate, modes, xt3, yt3, adv, out, held, done, sem):
    side = lanes((64, 128)) < 64
    for f in range(NF):
        scaled = [
            modes[4 * f + q] * jnp.where(side, rate[f, 2 * q], rate[f, 2 * q + 1]) for q in range(4)
        ]
        high, low = split(jnp.concatenate(scaled, axis=1))
        held[f] = dot(yt3[...], jnp.concatenate([high, high, low, low], axis=0))

    def write(f):
        return pltpu.make_async_copy(done.at[f], out.at[f], sem.at[f])

    for f in range(NF):
        rows = []
        for q in range(4):
            both = held[f, :, 128 * q : 128 * q + 128]
            rows += [jnp.where(side, both, 0.0), jnp.where(side, 0.0, both)]
        high, low = split(jnp.concatenate(rows, axis=0))
        tendency = dot(jnp.concatenate([high, low, high], axis=1), xt3[...])
        done[f] = adv[f] - tendency.reshape(NL, ROWS, COLS)
        write(f).start()
    for f in range(NF):
        write(f).wait()


def nudge(rate, modes, xt3, yt3, adv):
    vmem = pl.BlockSpec(memory_space=pltpu.VMEM)
    return pl.pallas_call(
        back_kernel,
        out_shape=jax.ShapeDtypeStruct((NF, NL, ROWS, COLS), F32),
        in_specs=[pl.BlockSpec(memory_space=pltpu.SMEM)] + [vmem] * 4,
        out_specs=pl.BlockSpec(memory_space=pltpu.HBM),
        scratch_shapes=[
            pltpu.VMEM((NF, 64, 512), F32),
            pltpu.VMEM((NF, NL, ROWS, COLS), F32),
            pltpu.SemaphoreType.DMA((NF,)),
        ],
        compiler_params=pltpu.CompilerParams(vmem_limit_bytes=32 * 1024 * 1024),
        name="nudge",
    )(rate, modes, xt3, yt3, adv)


def solution(mesh):
    tab_x, tab_y = tables()

    def on_device(state, driving, rate, sound_square):
        modes, adv, xt3, yt3 = sum_modes(state, driving, sound_square, jnp.asarray(tab_x), jnp.asarray(tab_y))
        return nudge(rate, modes.reshape(20, 64, 128), xt3, yt3, adv)

    return jax.shard_map(
        on_device,
        mesh=mesh,
        in_specs=(P(None, None, "gy", "gx"), P(None, None, "gy", "gx"), P(), P(None, "gy", "gx")),
        out_specs=P(None, None, "gy", "gx"),
        check_vma=False,
    )
```
